768 devices in a mesh: gx: 4 (over x), gy: 12 (over z), gz: 16 (over y, core).
Axes of the slice: x: 4, y: 8, z: 12, core: 2. Of those that a mesh axis runs over, the one named last changes fastest.
Arguments:
- conductivity: float32 [32, 96, 4096], P('gx', 'gy', 'gz'), may hold values from 0.1 to 10
- source: float32 [32, 96, 4096], P('gx', 'gy', 'gz'), may hold values from -5 to 5
Outputs:
- solution: float32 [32, 96, 4096], P('gx', 'gy', 'gz')
- residual: float32 [32, 96, 4096], P('gx', 'gy', 'gz')
The draws below stay inside these ranges and needn't reach their ends.
All inputs are finite; a program needn't handle non-finite values.
Results may differ from the reference program's by a relative error of at most 0.0003.
Values sent between devices are 32-bit elements; how exact they have to be, the bound alone decides.
A program may use at most 64 MiB of HBM per device.

```python
import math
import jax
import jax.numpy as jnp

LEVELS = 3
DEGREE = 4
COARSE_DEGREE = 8
NX = 32
NY = 96
NZ = 4096


def draw_source(key, part):
    rough = jnp.clip(jax.random.normal(key, (NX, NY, NZ), jnp.float32), -5.0, 5.0)
    return rough


def levels(stream_key, dims, cuts, smallest, largest):
    def one(position, parts):
        steps = jax.random.uniform(jax.random.fold_in(jax.random.fold_in(stream_key, 6), position), (parts,), jnp.float32, smallest / len(cuts), largest / len(cuts))
        return jnp.repeat(jnp.exp(steps), dims[position] // parts).reshape((-1,) + (1,) * (len(dims) - position - 1))

    factor_of = one(*cuts[0])
    for cut in cuts[1:]:
        factor_of = factor_of * one(*cut)
    return factor_of


def setup_inputs(seed: int = 0) -> dict:
    seeds = jax.random.split(jax.random.key(seed), 3)
    return {
        "conductivity": jnp.clip(jnp.exp(math.log(10.0) - 4.6051702 * jax.random.uniform(seeds[0], (NX, NY, NZ), jnp.float32) ** levels(seeds[0], (NX, NY, NZ), ((0, 4), (1, 12), (2, 16)), -0.2, 0.2)), 0.1, 10.0),
        "source": draw_source(jax.random.fold_in(seeds[2], 71), 0),
    }


weight_table = {1: 14.0 / 30.0, 2: 3.0 / 30.0, 3: 1.0 / 30.0}
neighbour_offsets = [(along_one, along_two, along_three) for along_one in (-1, 0, 1) for along_two in (-1, 0, 1) for along_three in (-1, 0, 1) if (along_one, along_two, along_three) != (0, 0, 0)]
smooth_low = 0.5
coarse_low = 0.03
upper_bound = 2.0


def shifted(padded, offset):
    return padded[1 + offset[0]:padded.shape[0] - 1 + offset[0], 1 + offset[1]:padded.shape[1] - 1 + offset[1], 1 + offset[2]:padded.shape[2] - 1 + offset[2]]


def stencil(field_pad, coeff_pad, spacing):
    centre_field = shifted(field_pad, (0, 0, 0))
    centre_coeff = shifted(coeff_pad, (0, 0, 0))
    total = jnp.zeros(centre_field.shape, jnp.float32)
    for offset in neighbour_offsets:
        weight = weight_table[abs(offset[0]) + abs(offset[1]) + abs(offset[2])]
        total = total + weight * (centre_coeff + shifted(coeff_pad, offset)) * (centre_field - shifted(field_pad, offset))
    return total * (0.5 / spacing)


def diagonal_of(coeff_pad, spacing):
    centre_coeff = shifted(coeff_pad, (0, 0, 0))
    total = jnp.zeros(centre_coeff.shape, jnp.float32)
    for offset in neighbour_offsets:
        weight = weight_table[abs(offset[0]) + abs(offset[1]) + abs(offset[2])]
        total = total + weight * (centre_coeff + shifted(coeff_pad, offset))
    return total * (0.5 / spacing)


def coarsen(values):
    extent = values.shape
    return values.reshape(extent[0] // 2, 2, extent[1] // 2, 2, extent[2] // 2, 2).mean(axis=(1, 3, 5))


def refine(values):
    return jnp.repeat(jnp.repeat(jnp.repeat(values, 2, axis=0), 2, axis=1), 2, axis=2)


def chebyshev_coefs(degree, lower):
    centre = (upper_bound + lower) / 2.0
    half_width = (upper_bound - lower) / 2.0
    ratio_term = centre / half_width
    rho_prev = 1.0 / ratio_term
    weights = []
    for number in range(1, degree):
        rho_next = 1.0 / (2.0 * ratio_term - rho_prev)
        weights.append((rho_next * rho_prev, 2.0 * rho_next / half_width))
        rho_prev = rho_next
    return centre, weights


def smooth(operate, diagonal, right_side, start, degree, lower, final):
    centre, weights = chebyshev_coefs(degree, lower)
    if start is None:
        residual = right_side
    else:
        residual = right_side - operate(start)
    update = residual / (centre * diagonal)
    solution = update if start is None else start + update
    for pair in weights:
        residual = residual - operate(update)
        update = pair[0] * update + pair[1] * residual / diagonal
        solution = solution + update
    if final:
        residual = residual - operate(update)
    return solution, residual


def reference(conductivity, source):
    coeffs = [conductivity]
    for number in range(1, LEVELS):
        coeffs.append(coarsen(coeffs[-1]))

    def cycle(grid_level, right_side):
        spacing = float(4 ** grid_level)
        coeff_pad = jnp.pad(coeffs[grid_level], 1)
        diagonal = diagonal_of(coeff_pad, spacing)

        def operate(field):
            return stencil(jnp.pad(field, 1), coeff_pad, spacing)

        if grid_level == LEVELS - 1:
            return smooth(operate, diagonal, right_side, None, COARSE_DEGREE, coarse_low, False)
        solution, residual = smooth(operate, diagonal, right_side, None, DEGREE, smooth_low, True)
        correction, ignored = cycle(grid_level + 1, coarsen(residual))
        solution = solution + refine(correction)
        return smooth(operate, diagonal, right_side, solution, DEGREE, smooth_low, grid_level == 0)

    return cycle(0, source)
```

```python
import jax
import jax.numpy as jnp
from jax import lax
from jax.experimental import pallas as pl
from jax.experimental.pallas import tpu as pltpu
from jax.sharding import PartitionSpec as P

MESH = pl.DeviceIdType.MESH
F32 = jnp.float32
DEGREE = 4
COARSE_DEGREE = 8
UPPER = 2.0
FINE_LOW = 0.5
COARSE_LOW = 0.03
REACH = 5
SPAN = 2 * REACH + 1

P0, W0 = 5, 8
P1, W1 = 4, 8
P2, W2 = 2, 18
SIDES = (-1, 0, 1)
FLAT = [(i, j, 0) for i in SIDES for j in SIDES if (i, j) != (0, 0)]
STACK = [(i, j, k) for k in (-1, 1) for i in SIDES for j in SIDES]
AROUND = STACK + sorted(FLAT, key=lambda o: -abs(o[0]) - abs(o[1]))


def chebyshev_coefs(degree, lower):
    centre = (UPPER + lower) / 2.0
    half_width = (UPPER - lower) / 2.0
    ratio_term = centre / half_width
    rho_prev = 1.0 / ratio_term
    weights = []
    for _ in range(1, degree):
        rho_next = 1.0 / (2.0 * ratio_term - rho_prev)
        weights.append((rho_next * rho_prev, 2.0 * rho_next / half_width))
        rho_prev = rho_next
    return 1.0 / centre, weights


def rolled(values, shift):
    flat = values.reshape(-1, 128)
    return pltpu.roll(flat, shift % 128, 1).reshape(values.shape)


def lanes_of(shape):
    return lax.broadcasted_iota(jnp.int32, shape, len(shape) - 1)


def beside(values):
    up, down = rolled(values, 1), rolled(values, -1)
    tiles = values.shape[1]
    if tiles > 1:
        lane = lanes_of(values.shape)
        before = jnp.concatenate([up[:, tiles - 1 :], up[:, : tiles - 1]], axis=1)
        after = jnp.concatenate([down[:, 1:], down[:, :1]], axis=1)
        up = jnp.where(lane == 0, before, up)
        down = jnp.where(lane == 127, after, down)
    return up + down


def stencil_sum(ref, first, count, row, rows):
    planes = pl.ds(first - 1, count + 2)
    centre = ref[planes, :, pl.ds(row, rows), :]
    side = ref[planes, :, pl.ds(row - 1, rows), :] + ref[planes, :, pl.ds(row + 1, rows), :]
    corner = 3.0 * centre + side
    face = 14.0 * centre + 3.0 * side
    outer = face[1:-1] + corner[:-2] + corner[2:]
    middle = 14.0 * side[1:-1] + face[:-2] + face[2:]
    return middle + beside(outer)


def chunks(first, last, size):
    return [(at, min(size, last - at)) for at in range(first, last, size)]


def apply(level, source, r_in, r_out, planes, row, rows, coefs, target=None, tiles=None, keep=None, size=2):
    kappa, diagonal, inverse = level
    v_ref, w_ref = source
    for first, count in chunks(planes[0], planes[1], size):
        at = (pl.ds(first, count), slice(None), pl.ds(row, rows), slice(None))
        v = v_ref[at]
        r = r_in(at) - diagonal[at] * v
        r = r + kappa[at] * stencil_sum(v_ref, first, count, row, rows)
        r = r + stencil_sum(w_ref, first, count, row, rows)
        if r_out is not None:
            r_out(first, count, r)
        if coefs is not None:
            new = (coefs[1] * inverse[at]) * r
            if coefs[0] is not None:
                new = new + coefs[0] * v
            target[0][at] = new
            if target[1] is not None:
                target[1][at] = kappa[at] * new


def pair_gather(values, index):
    return jnp.take_along_axis(values, index, axis=1)


def kernel(sizes, k_ref, b_ref, x_ref, r_ref, ext, edge_in, edge_out, redge_in, redge_out, rext,
           kap0, dia0, inv0, res0, va0, wa0, vb0, wb0, xs0,
           kin1, bin1, kap1, dia1, inv1, res1, va1, wa1, vb1, wb1, rex1, xex1, xs1,
           kap2, dia2, inv2, bin2, res2, va2, wa2, vb2, wb2, xs2, tmp, tmp2, send, recv):
    nx, ny, nz = sizes
    mx, my, mz = lax.axis_index("gx"), lax.axis_index("gy"), lax.axis_index("gz")
    used = [0]
    pending = []

    def inside(i, j, k):
        tests = []
        if i < 0:
            tests.append(mx + i >= 0)
        if i > 0:
            tests.append(mx + i < nx)
        if j < 0:
            tests.append(my + j >= 0)
        if j > 0:
            tests.append(my + j < ny)
        if k < 0:
            tests.append(mz + k >= 0)
        if k > 0:
            tests.append(mz + k < nz)
        ok = tests[0]
        for test in tests[1:]:
            ok = ok & test
        return ok

    def exchange(offsets, ends):
        base = used[0]
        used[0] += len(offsets)
        copies = []
        for n, (i, j, k) in enumerate(offsets):
            src, dst = ends(i, j, k)
            copy = pltpu.make_async_remote_copy(
                src_ref=src, dst_ref=dst, send_sem=send.at[base + n], recv_sem=recv.at[base + n],
                device_id=(mx + i, my + j, mz + k), device_id_type=MESH,
            )
            ok = inside(i, j, k)
            pl.when(ok)(copy.start)
            pending.append((ok, copy))
            copies.append((inside(-i, -j, -k), copy))

        def arrive():
            for ok, copy in copies:
                pl.when(ok)(copy.wait_recv)

        return arrive

    def plane_gather(ref):
        base = used[0]
        used[0] += nx * SPAN
        arrivals = []
        for j in sorted(range(-REACH, REACH + 1), key=lambda o: -abs(o)):
            if abs(j) >= ny:
                continue
            for gx in range(nx):
                ok = gx != mx if j == 0 else inside(0, j, 0)
                mine = (pl.ds(P2 + 2 * mx, 2), slice(None), pl.ds(W2, 2), slice(None))
                there = (pl.ds(P2 + 2 * mx, 2), slice(None), pl.ds(W2 - 2 * j, 2), slice(None))
                copy = pltpu.make_async_remote_copy(
                    src_ref=ref.at[mine], dst_ref=ref.at[there],
                    send_sem=send.at[base + gx * SPAN + j + REACH], recv_sem=recv.at[base + mx * SPAN + j + REACH],
                    device_id=(gx, my + j, mz), device_id_type=MESH,
                )
                pl.when(ok)(copy.start)
                pending.append((ok, copy))
                back = pltpu.make_async_remote_copy(
                    src_ref=ref.at[mine], dst_ref=ref.at[there],
                    send_sem=send.at[base + gx * SPAN + j + REACH], recv_sem=recv.at[base + gx * SPAN + j + REACH],
                    device_id=(gx, my, mz), device_id_type=MESH,
                )
                arrivals.append((gx != mx if j == 0 else inside(0, -j, 0), back))

        def arrive():
            for ok, copy in arrivals:
                pl.when(ok)(copy.wait_recv)

        return arrive

    def zero(ref):
        ref[...] = jnp.zeros(ref.shape, F32)

    def coarse_of(read, count, rows):
        for tile in range(2):
            for i in range(count):
                total = read(2 * i, 0, tile) + read(2 * i, 1, tile) + read(2 * i + 1, 0, tile) + read(2 * i + 1, 1, tile)
                tmp[tile, rows * i : rows * (i + 1), :] = 0.125 * total
        size = max(8, count * rows)
        lane = lanes_of((size, 128))
        pairs = [tmp[tile, 0:size, :] for tile in range(2)]
        pairs = [p + pltpu.roll(p, 127, 1) for p in pairs]
        index = (2 * lane) % 128
        out = jnp.where(lane < 64, pair_gather(pairs[0], index), pair_gather(pairs[1], index))
        tmp2[0:size, :] = out
        return [tmp2[rows * i : rows * (i + 1), :] for i in range(count)]

    def pack_edges(reads, out):
        for way, (tile, start) in enumerate(((1, 120), (0, 0))):
            packed = jnp.zeros((8, 128), F32)
            lane = lanes_of((8, 128))
            for a, read in enumerate(reads):
                for i in range(8):
                    at = 8 * i + 64 * a
                    part = pltpu.roll(read(i, tile), (at - start) % 128, 1)
                    packed = jnp.where((lane >= at) & (lane < at + 8), part, packed)
            out[way] = packed

    def edge_ends(src, dst):
        def ends(i, j, k):
            way, side = (0, 0) if k > 0 else (1, 1)
            return src.at[way], dst.at[side, 1 - i, pl.ds(8 * (1 - j), 8), :]

        return ends

    def unpack_edges(src, a, write):
        lane = lanes_of((24, 128))
        for p in range(2 * P0 + 8):
            group, i = (0, 3 + p) if p < P0 else ((1, p - P0) if p < P0 + 8 else (2, p - P0 - 8))
            at = 8 * i + 64 * a
            low = pltpu.roll(src[0, group], (120 - at) % 128, 1)
            high = pltpu.roll(src[1, group], -at % 128, 1)
            write(p, jnp.where(lane < 8, high, jnp.where(lane >= 120, low, 0.0)))

    def fine_slices(i, j):
        src_planes = {1: pl.ds(P0 + 3, 5), 0: pl.ds(P0, 8), -1: pl.ds(P0, 5)}[i]
        dst_planes = {1: pl.ds(0, 5), 0: pl.ds(P0, 8), -1: pl.ds(P0 + 8, 5)}[i]
        src_rows = {1: pl.ds(W0 + 3, 5), 0: pl.ds(W0, 8), -1: pl.ds(W0, 5)}[j]
        dst_rows = {1: pl.ds(W0 - 5, 5), 0: pl.ds(W0, 8), -1: pl.ds(W0 + 8, 5)}[j]
        return (src_planes, pl.ds(0, 2), src_rows), (dst_planes, pl.ds(0, 2), dst_rows)

    def coarse_slices(i, j):
        return (pl.ds(P1, 4), pl.ds(W1, 4)), (pl.ds(P1 - 4 * i, 4), pl.ds(W1 - 4 * j, 4))

    def level1_ends(ref):
        def ends(i, j, k):
            (sp, sr), (dp, dr) = coarse_slices(i, j)
            slot = {0: 0, -1: 1, 1: 2}[k]
            return ref.at[0, sp, sr, :], ref.at[slot, dp, dr, :]

        return ends

    def flat1_ends(ref):
        def ends(i, j, k):
            (sp, sr), (dp, dr) = coarse_slices(i, j)
            return ref.at[sp, :, sr, :], ref.at[dp, :, dr, :]

        return ends

    for ref in (ext, edge_in, kin1, kap2, bin2):
        zero(ref)
    for tile in range(2):
        cols = slice(128 * tile, 128 * tile + 128)
        ext[0, P0 : P0 + 8, tile, W0 : W0 + 8, :] = b_ref[:, :, cols]
        ext[1, P0 : P0 + 8, tile, W0 : W0 + 8, :] = k_ref[:, :, cols]

    barrier = pltpu.get_barrier_semaphore()

    def greet(ok, i, j, k):
        @pl.when(ok)
        def _():
            pl.semaphore_signal(barrier, inc=1, device_id=(i, j, k), device_id_type=MESH)

        return jnp.where(ok, 1, 0)

    count = 0
    for i, j, k in STACK:
        count = count + greet(inside(i, j, k), mx + i, my + j, mz + k)
    for j in range(-REACH, REACH + 1):
        if abs(j) < ny:
            for gx in range(nx):
                count = count + greet(gx != mx if j == 0 else inside(0, j, 0), gx, my + j, mz)

    for ref in (redge_in, rext, va0, wa0, vb0, wb0, bin1, dia1, va1, wa1, vb1, wb1, rex1, xex1, va2, wa2, vb2, wb2, xs2, tmp):
        zero(ref)
    pack_edges([lambda i, t: ext[0, P0 + i, t, W0 : W0 + 8, :], lambda i, t: ext[1, P0 + i, t, W0 : W0 + 8, :]], edge_out)
    own_k1 = coarse_of(lambda i, parity, t: ext[1, P0 + i, t, pl.ds(W0 + parity, 4, stride=2), :], 4, 4)
    for i, value in enumerate(own_k1):
        kin1[0, P1 + i, W1 : W1 + 4, :] = value

    pl.semaphore_wait(barrier, count)

    edges_arrive = exchange(STACK, edge_ends(edge_out, edge_in))

    def fine_ends(i, j, k):
        (sp, st, sr), (dp, dt, dr) = fine_slices(i, j)
        return ext.at[:, sp, st, sr, :], ext.at[:, dp, dt, dr, :]

    fine_arrive = exchange(sorted(FLAT, key=lambda o: -abs(o[0]) - abs(o[1])), fine_ends)
    k1_arrive = exchange(AROUND, level1_ends(kin1))
    edges_arrive()
    fine_arrive()

    def put(a):
        def write(p, value):
            ext[a, p, 2] = value

        return write

    unpack_edges(edge_in, 0, put(0))
    unpack_edges(edge_in, 1, put(1))
    for first, n in chunks(0, 18, 3):
        kap0[first : first + n] = ext[1, first : first + n] * (0.5 / 30.0)
    theta0, weights0 = chebyshev_coefs(DEGREE, FINE_LOW)
    lo, hi = P0 - 4, P0 + 12

    def start_level(level, planes, row, rows, theta, r_in, v_ref, w_ref, make_diagonal, size=2):
        kappa, diagonal, inverse = level
        for first, n in chunks(planes[0], planes[1], size):
            at = (pl.ds(first, n), slice(None), pl.ds(row, rows), slice(None))
            kap = kappa[at]
            if make_diagonal:
                dia = 128.0 * kap + stencil_sum(kappa, first, n, row, rows)
                diagonal[at] = dia
            else:
                dia = diagonal[at]
            inv = jnp.where(kap > 0.0, 1.0 / dia, 0.0)
            inverse[at] = inv
            new = (theta * inv) * r_in(at)
            v_ref[at] = new
            w_ref[at] = kap * new

    level0 = (kap0, dia0, inv0)
    start_level(level0, (lo, hi), 4, 16, theta0, lambda at: ext[(0,) + at], va0, wa0, True)

    def own0(ref):
        return ref[P0 : P0 + 8, 0:2, W0 : W0 + 8, :]

    def put_res0(first, n, r):
        res0[pl.ds(first, n), :, 4:20, :] = r

    xs0[...] = own0(va0)
    here, there = (va0, wa0), (vb0, wb0)

    def smooth0(step, r_in):
        nonlocal here, there
        apply(level0, here, r_in, put_res0, (P0 - 3 + step, P0 + 11 - step), 4, 16, weights0[step], there)
        xs0[...] += own0(there[0])
        here, there = there, here

    smooth0(0, lambda at: ext[(0,) + at])

    k1_arrive()
    for first, n in chunks(0, 12, 2):
        kap1[first : first + n, 0] = kin1[0, first : first + n] * (0.125 / 30.0)
        lane = lanes_of((n, 24, 128))
        halo = jnp.where(lane < 64, kin1[1, first : first + n], kin1[2, first : first + n])
        kap1[first : first + n, 1] = halo * (0.125 / 30.0)
    for first, n in chunks(P1, P1 + 4, 2):
        at = (pl.ds(first, n), slice(None), pl.ds(W1, 8), slice(None))
        value = 128.0 * kap1[at] + stencil_sum(kap1, first, n, W1, 8)
        dia1[first : first + n, :, W1 : W1 + 4, :] = value[:, :, 0:4]
    dia1_arrive = exchange(FLAT, flat1_ends(dia1))
    own_k2 = coarse_of(lambda i, parity, t: kap1[P1 + i, t, pl.ds(W1 + parity, 2, stride=2), :], 2, 2)
    for i, value in enumerate(own_k2):
        kap2[P2 + 2 * mx + i, 0, W2 : W2 + 2, :] = 0.25 * value
    k2_arrive = plane_gather(kap2)

    smooth0(1, lambda at: res0[at])
    smooth0(2, lambda at: res0[at])

    def put_rext(first, n, r):
        rext[pl.ds(first, n), 0:2, W0 : W0 + 8, :] = r[:, 0:2]

    apply(level0, here, lambda at: res0[at], put_rext, (P0, P0 + 8), W0, 8, None)

    own_b1 = coarse_of(lambda i, parity, t: rext[P0 + i, t, pl.ds(W0 + parity, 4, stride=2), :], 4, 4)
    for i, value in enumerate(own_b1):
        bin1[0, P1 + i, W1 : W1 + 4, :] = value
    b1_arrive = exchange(AROUND, level1_ends(bin1))
    pack_edges([lambda i, t: rext[P0 + i, t, W0 : W0 + 8, :]], redge_out)
    redges_arrive = exchange(STACK, edge_ends(redge_out, redge_in))

    def rext_ends(i, j, k):
        (sp, st, sr), (dp, dt, dr) = fine_slices(i, j)
        return rext.at[sp, st, sr, :], rext.at[dp, dt, dr, :]

    rext_arrive = exchange(FLAT, rext_ends)
    dia1_arrive()
    b1_arrive()
    for first, n in chunks(0, 12, 2):
        res1[first : first + n, 0] = bin1[0, first : first + n]
        lane = lanes_of((n, 24, 128))
        res1[first : first + n, 1] = jnp.where(lane < 64, bin1[1, first : first + n], bin1[2, first : first + n])
    level1 = (kap1, dia1, inv1)
    start_level(level1, (0, 12), 4, 16, theta0, lambda at: res1[at], va1, wa1, False)

    def own1(ref):
        return ref[P1 : P1 + 4, :, W1 : W1 + 8, :]

    def put_res1(first, n, r):
        res1[pl.ds(first, n), :, 4:20, :] = r

    xs1[...] = own1(va1)
    here, there = (va1, wa1), (vb1, wb1)
    for step in range(3):
        apply(level1, here, lambda at: res1[at], put_res1, (P1 - 3 + step, P1 + 7 - step), 4, 16, weights0[step], there)
        xs1[...] += own1(there[0])
        here, there = there, here

    def put_rex1(first, n, r):
        rex1[pl.ds(first, n), :, W1 : W1 + 4, :] = r[:, :, 0:4]

    apply(level1, here, lambda at: res1[at], put_rex1, (P1, P1 + 4), W1, 8, None)

    own_b2 = coarse_of(lambda i, parity, t: rex1[P1 + i, t, pl.ds(W1 + parity, 2, stride=2), :], 2, 2)
    for i, value in enumerate(own_b2):
        bin2[P2 + 2 * mx + i, 0, W2 : W2 + 2, :] = value
    b2_arrive = plane_gather(bin2)
    rex1_arrive = exchange(FLAT, flat1_ends(rex1))
    k2_arrive()
    full = 2 * nx
    theta2, weights2 = chebyshev_coefs(COARSE_DEGREE, COARSE_LOW)
    level2 = (kap2, dia2, inv2)
    b2_arrive()
    start_level(level2, (P2, P2 + full), 8, 24, theta2, lambda at: bin2[at], va2, wa2, True)
    window = (slice(P2, P2 + full), slice(None), slice(8, 32), slice(None))
    xs2[window] = va2[window]
    here, there = (va2, wa2), (vb2, wb2)

    def put_res2(first, n, r):
        res2[pl.ds(first, n), :, 8:32, :] = r

    for step in range(COARSE_DEGREE - 1):
        r_in = (lambda at: bin2[at]) if step == 0 else (lambda at: res2[at])
        apply(level2, here, r_in, put_res2, (P2, P2 + full), 8, 24, weights2[step], there)
        xs2[window] += there[0][window]
        here, there = there, here

    half = lanes_of((8, 128)) // 2
    for j in range(6):
        coarse = xs2[P2 + 2 * mx - 2 + j, 0, W2 - 2 : W2 + 6, :]
        for tile in range(2):
            value = pair_gather(coarse, half + 64 * tile)[0:6]
            for e in range(2):
                for parity in range(2):
                    va1[2 * j + e, tile, pl.ds(W1 - 4 + parity, 6, stride=2), :] = value
    for first, n in chunks(0, 12, 2):
        wa1[first : first + n] = kap1[first : first + n] * va1[first : first + n]
    xs1[...] += own1(va1)
    rex1_arrive()
    here, there = (va1, wa1), (vb1, wb1)
    apply(level1, here, lambda at: rex1[at], put_res1, (P1 - 3, P1 + 7), 4, 16, (None, theta0), there)
    xs1[...] += own1(there[0])
    here, there = there, here
    for step in range(3):
        apply(level1, here, lambda at: res1[at], put_res1, (P1 - 2 + step, P1 + 6 - step), 4, 16, weights0[step], there)
        xs1[...] += own1(there[0])
        here, there = there, here
    xex1[P1 : P1 + 4, :, W1 : W1 + 4, :] = xs1[:, :, 0:4, :]
    xex1_arrive = exchange(FLAT, flat1_ends(xex1))

    redges_arrive()

    def put_rext2(p, value):
        rext[p, 2] = value

    unpack_edges(redge_in, 0, put_rext2)
    rext_arrive()
    xex1_arrive()
    lane = lanes_of((8, 128))
    ends = jnp.where(lane < 64, half, half + 64)
    for p in range(1, 11):
        for source_row, keep in ((W1 - 4, 8), (W1 + 4, 4)):
            for tile, source_tile, index in ((0, 0, half), (1, 0, half + 64), (2, 1, ends)):
                value = pair_gather(xex1[p, source_tile, source_row : source_row + 8, :], index)[0:keep]
                for q in (2 * p - 3, 2 * p - 2):
                    if 0 <= q < 18:
                        for parity in range(2):
                            va0[q, tile, pl.ds(2 * (source_row - 4) + parity, keep, stride=2), :] = value
    for first, n in chunks(0, 18, 2):
        wa0[first : first + n] = kap0[first : first + n] * va0[first : first + n]
    xs0[...] += own0(va0)
    here, there = (va0, wa0), (vb0, wb0)
    apply(level0, here, lambda at: rext[at], put_res0, (lo, hi), 4, 16, (None, theta0), there)
    xs0[...] += own0(there[0])
    here, there = there, here
    for step in range(3):
        smooth0(step, lambda at: res0[at])

    def put_out(first, n, r):
        for tile in range(2):
            r_ref[first - P0 : first - P0 + n, :, 128 * tile : 128 * tile + 128] = r[:, tile]

    apply(level0, here, lambda at: res0[at], put_out, (P0, P0 + 8), W0, 8, None)
    for tile in range(2):
        x_ref[:, :, 128 * tile : 128 * tile + 128] = xs0[:, tile]
    for ok, copy in pending:
        pl.when(ok)(copy.wait_send)


def solution(mesh):
    sizes = tuple(mesh.shape[axis] for axis in ("gx", "gy", "gz"))

    def step(conductivity, source):
        def vmem(*shape):
            return pltpu.VMEM(shape, F32)

        level0, level1, level2 = (18, 3, 24, 128), (12, 2, 24, 128), (12, 1, 40, 128)
        sems = 4 * 26 + 3 * 8 + 2 * sizes[0] * SPAN
        shape = jax.ShapeDtypeStruct(conductivity.shape, F32)
        return pl.pallas_call(
            lambda *refs: kernel(sizes, *refs),
            name="cycle",
            out_shape=(shape, shape),
            in_specs=[pl.BlockSpec(memory_space=pltpu.VMEM)] * 2,
            out_specs=(pl.BlockSpec(memory_space=pltpu.VMEM),) * 2,
            scratch_shapes=[
                vmem(2, *level0), vmem(2, 3, 24, 128), vmem(2, 8, 128), vmem(2, 3, 24, 128), vmem(2, 8, 128), vmem(*level0),
                *[vmem(*level0) for _ in range(8)], vmem(8, 2, 8, 128),
                vmem(3, 12, 24, 128), vmem(3, 12, 24, 128), *[vmem(*level1) for _ in range(10)], vmem(4, 2, 8, 128),
                *[vmem(*level2) for _ in range(10)],
                vmem(2, 16, 128), vmem(16, 128),
                pltpu.SemaphoreType.DMA((sems,)), pltpu.SemaphoreType.DMA((sems,)),
            ],
            compiler_params=pltpu.CompilerParams(
                collective_id=0, has_side_effects=True, vmem_limit_bytes=50 * 1024 * 1024
            ),
        )(conductivity, source)

    spec = P("gx", "gy", "gz")
    return jax.shard_map(step, mesh=mesh, in_specs=(spec, spec), out_specs=(spec, spec), check_vma=False)
```

```python
import jax
import jax.numpy as jnp
from jax import lax
from jax.experimental import pallas as pl
from jax.experimental.pallas import tpu as pltpu
from jax.sharding import PartitionSpec as P

MESH = pl.DeviceIdType.MESH
F32 = jnp.float32
DEGREE = 4
COARSE_DEGREE = 8
UPPER = 2.0
FINE_LOW = 0.5
COARSE_LOW = 0.03
REACH = 5

P0, W0 = 5, 8
P1, W1 = 4, 8
P2, W2 = 2, 18
SIDES = (-1, 0, 1)
FLAT = [(i, j, 0) for i in SIDES for j in SIDES if (i, j) != (0, 0)]
STACK = [(i, j, k) for k in (-1, 1) for i in SIDES for j in SIDES]
DIAGONAL_FIRST = sorted(FLAT, key=lambda o: -abs(o[0]) - abs(o[1]))


def chebyshev_coefs(degree, lower):
    centre = (UPPER + lower) / 2.0
    half_width = (UPPER - lower) / 2.0
    ratio_term = centre / half_width
    rho_prev = 1.0 / ratio_term
    weights = []
    for _ in range(1, degree):
        rho_next = 1.0 / (2.0 * ratio_term - rho_prev)
        weights.append((rho_next * rho_prev, 2.0 * rho_next / half_width))
        rho_prev = rho_next
    return 1.0 / centre, weights


def rolled(values, shift):
    flat = values.reshape(-1, 128)
    return pltpu.roll(flat, shift % 128, 1).reshape(values.shape)


def lanes_of(shape):
    return lax.broadcasted_iota(jnp.int32, shape, len(shape) - 1)


def beside(values):
    up, down = rolled(values, 1), rolled(values, -1)
    tiles = values.shape[1]
    if tiles > 1:
        lane = lanes_of(values.shape)
        before = jnp.concatenate([up[:, tiles - 1 :], up[:, : tiles - 1]], axis=1)
        after = jnp.concatenate([down[:, 1:], down[:, :1]], axis=1)
        up = jnp.where(lane == 0, before, up)
        down = jnp.where(lane == 127, after, down)
    return up + down


def stencil_sum(ref, first, count, row, rows):
    planes = pl.ds(first - 1, count + 2)
    centre = ref[planes, :, pl.ds(row, rows), :]
    side = ref[planes, :, pl.ds(row - 1, rows), :] + ref[planes, :, pl.ds(row + 1, rows), :]
    corner = 3.0 * centre + side
    face = 14.0 * centre + 3.0 * side
    outer = face[1:-1] + corner[:-2] + corner[2:]
    middle = 14.0 * side[1:-1] + face[:-2] + face[2:]
    return middle + beside(outer)


def chunks(first, last, size):
    return [(at, min(size, last - at)) for at in range(first, last, size)]


def apply(level, source, r_in, r_out, planes, row, rows, coefs, target=None, size=2):
    kappa, diagonal, inverse = level
    v_ref, w_ref = source
    for first, count in chunks(planes[0], planes[1], size):
        at = (pl.ds(first, count), slice(None), pl.ds(row, rows), slice(None))
        v = v_ref[at]
        r = r_in(at) - diagonal[at] * v
        r = r + kappa[at] * stencil_sum(v_ref, first, count, row, rows)
        r = r + stencil_sum(w_ref, first, count, row, rows)
        if r_out is not None:
            r_out(first, count, r)
        if coefs is not None:
            new = (coefs[1] * inverse[at]) * r
            if coefs[0] is not None:
                new = new + coefs[0] * v
            target[0][at] = new
            target[1][at] = kappa[at] * new


def pair_gather(values, index):
    return jnp.take_along_axis(values, index, axis=1)


def kernel(sizes, k_ref, b_ref, x_ref, r_ref, ext, edge_in, edge_out, redge_in, redge_out, rext,
           kap0, dia0, inv0, res0, va0, wa0, vb0, wb0, xs0,
           kin1, bin1, kedge_in, kedge_out, bedge_in, bedge_out, kap1, dia1, inv1, res1, va1, wa1, vb1, wb1, rex1, xex1, xs1,
           kin2, kap2, dia2, inv2, bin2, res2, va2, wa2, vb2, wb2, xs2, tmp, tmp2, spare, send, recv, load):
    nx, ny, nz = sizes
    mx, my, mz = lax.axis_index("gx"), lax.axis_index("gy"), lax.axis_index("gz")
    used = [0]

    def inside(i, j, k):
        tests = []
        if i < 0:
            tests.append(mx + i >= 0)
        if i > 0:
            tests.append(mx + i < nx)
        if j < 0:
            tests.append(my + j >= 0)
        if j > 0:
            tests.append(my + j < ny)
        if k < 0:
            tests.append(mz + k >= 0)
        if k > 0:
            tests.append(mz + k < nz)
        ok = tests[0]
        for test in tests[1:]:
            ok = ok & test
        return ok

    def amount(where, rows, number, sent):
        whole = spare.at[pl.ds(0, rows)]

        @pl.when(where)
        def _():
            copy = pltpu.make_async_remote_copy(
                src_ref=whole, dst_ref=whole, send_sem=send.at[number], recv_sem=recv.at[number],
                device_id=(mx, my, mz), device_id_type=MESH,
            )
            if sent:
                copy.wait_send()
            else:
                copy.wait_recv()

    def waits(number, cases):
        def wait(sent):
            with jax.named_scope(f"{'sent' if sent else 'wait'}{number}"):
                for where, rows in cases:
                    amount(where, rows, number, sent)

        return (lambda: wait(False)), (lambda: wait(True))

    def some(n):
        return (1, 2) if n > 2 else (1,)

    near_x = jnp.where(mx > 0, 1, 0) + jnp.where(mx < nx - 1, 1, 0)
    near_y = jnp.where(my > 0, 1, 0) + jnp.where(my < ny - 1, 1, 0)
    near_z = jnp.where(mz > 0, 1, 0) + jnp.where(mz < nz - 1, 1, 0)
    low_y, high_y = jnp.minimum(my, REACH), jnp.minimum(ny - 1 - my, REACH)
    far_counts = sorted({min(y, REACH) + min(ny - 1 - y, REACH) for y in range(ny)})

    def exchange(moves, face, corner, stack):
        number = used[0]
        used[0] += 1
        for (i, j, k), src, dst in moves:
            copy = pltpu.make_async_remote_copy(
                src_ref=src, dst_ref=dst, send_sem=send.at[number], recv_sem=recv.at[number],
                device_id=(mx + i, my + j, mz + k), device_id_type=MESH,
            )
            pl.when(inside(i, j, k))(copy.start)
        cases = []
        for x in some(nx):
            for y in some(ny):
                for z in some(nz) if stack else (0,):
                    where = (near_x == x) & (near_y == y)
                    if stack:
                        where = where & (near_z == z)
                    cases.append((where, (x + y) * face + x * y * corner + z * (1 + x) * (1 + y) * stack))
        return waits(number, cases)

    def mine(ref):
        return ref.at[pl.ds(P2 + 2 * mx, 2), :, pl.ds(W2, 2), :]

    def far_start(ref, number, shift, j):
        copy = pltpu.make_async_remote_copy(
            src_ref=mine(ref), dst_ref=ref.at[pl.ds(P2 + 2 * mx, 2), :, pl.ds(W2 - 2 * j, 2), :],
            send_sem=send.at[number], recv_sem=recv.at[number],
            device_id=(lax.rem(mx + shift, nx), my + j, mz), device_id_type=MESH,
        )
        if j == 0:
            copy.start()
        else:
            pl.when(inside(0, j, 0))(copy.start)

    distances = [j for j in sorted(range(-REACH, REACH + 1), key=lambda o: -abs(o)) if abs(j) < ny]

    def column_gather(ref):
        number = used[0]
        used[0] += 1
        for j in distances:
            if j != 0:
                far_start(ref, number, 0, j)
        return waits(number, [(low_y + high_y == c, 4 * c) for c in far_counts])

    def plane_gather(ref):
        number = used[0]
        used[0] += 1
        for j in distances:
            for shift in range(nx):
                if (shift, j) != (0, 0):
                    far_start(ref, number, shift, j)
        return waits(number, [(low_y + high_y == c, 4 * ((1 + c) * nx - 1)) for c in far_counts])

    def row_gather(ref):
        number = used[0]
        used[0] += 1
        part = ref.at[pl.ds(P2 + 2 * mx, 2), :, pl.ds(W2 - 2 * REACH, 4 * REACH + 2), :]
        for shift in range(1, nx):
            pltpu.make_async_remote_copy(
                src_ref=part, dst_ref=part, send_sem=send.at[number], recv_sem=recv.at[number],
                device_id=(lax.rem(mx + shift, nx), my, mz), device_id_type=MESH,
            ).start()
        return waits(number, [(mx >= 0, (nx - 1) * 2 * (4 * REACH + 2))])

    def zero(ref):
        ref[...] = jnp.zeros(ref.shape, F32)

    def coarse_of(read, count, rows):
        for tile in range(2):
            for i in range(count):
                total = read(2 * i, 0, tile) + read(2 * i, 1, tile) + read(2 * i + 1, 0, tile) + read(2 * i + 1, 1, tile)
                tmp[tile, rows * i : rows * (i + 1), :] = 0.125 * total
        size = max(8, count * rows)
        lane = lanes_of((size, 128))
        pairs = [tmp[tile, 0:size, :] for tile in range(2)]
        pairs = [p + pltpu.roll(p, 127, 1) for p in pairs]
        index = (2 * lane) % 128
        out = jnp.where(lane < 64, pair_gather(pairs[0], index), pair_gather(pairs[1], index))
        tmp2[0:size, :] = out
        return [tmp2[rows * i : rows * (i + 1), :] for i in range(count)]

    def pack_edges(reads, out):
        for way, (tile, start) in enumerate(((1, 120), (0, 0))):
            packed = jnp.zeros((8, 128), F32)
            lane = lanes_of((8, 128))
            for a, read in enumerate(reads):
                for i in range(8):
                    at = 8 * i + 64 * a
                    part = pltpu.roll(read(i, tile), (at - start) % 128, 1)
                    packed = jnp.where((lane >= at) & (lane < at + 8), part, packed)
            out[way] = packed

    def edge_moves(src, dst, width):
        moves = []
        for i, j, k in STACK:
            way, side = (0, 0) if k > 0 else (1, 1)
            own = W0 if width == 8 else W1
            to = dst.at[side, 1 - i, pl.ds(own - width * j, width), :]
            moves.append(((i, j, k), src.at[way, pl.ds(0, width), :], to))
        return moves

    def pack_coarse(out):
        lane = lanes_of((4, 128))
        for way, start in enumerate((96, 0)):
            packed = jnp.zeros((4, 128), F32)
            for i in range(4):
                part = pltpu.roll(tmp2[4 * i : 4 * i + 8, :], (32 * i - start) % 128, 1)[0:4]
                packed = jnp.where((lane >= 32 * i) & (lane < 32 * i + 32), part, packed)
            out[way, 0:4] = packed

    def unpack_coarse(src, p):
        lane = lanes_of((24, 128))
        high_end, low_start = jnp.where(mz < nz - 1, 32, 0), jnp.where(mz > 0, 96, 128)
        low = pltpu.roll(src[0, p // 4], (96 - 32 * (p % 4)) % 128, 1)
        high = pltpu.roll(src[1, p // 4], (-32 * (p % 4)) % 128, 1)
        return jnp.where(lane < high_end, high, jnp.where(lane >= low_start, low, 0.0))

    def unpack_edges(src, a, write):
        lane = lanes_of((24, 128))
        high_end, low_start = jnp.where(mz < nz - 1, 8, 0), jnp.where(mz > 0, 120, 128)
        for p in range(2 * P0 + 8):
            group, i = (0, 3 + p) if p < P0 else ((1, p - P0) if p < P0 + 8 else (2, p - P0 - 8))
            at = 8 * i + 64 * a
            low = pltpu.roll(src[0, group], (120 - at) % 128, 1)
            high = pltpu.roll(src[1, group], -at % 128, 1)
            write(p, jnp.where(lane < high_end, high, jnp.where(lane >= low_start, low, 0.0)))

    def halo(step, own, width, depth):
        if step == 0:
            return pl.ds(own, width), pl.ds(own, width)
        if step > 0:
            return pl.ds(own + width - depth, depth), pl.ds(own - depth, depth)
        return pl.ds(own, depth), pl.ds(own + width, depth)

    def fine_moves(ref, depth):
        moves = []
        for i, j, k in DIAGONAL_FIRST:
            (sp, dp), (sr, dr) = halo(i, P0, 8, depth), halo(j, W0, 8, depth)
            moves.append(((i, j, k), ref.at[sp, pl.ds(0, 2), sr, :], ref.at[dp, pl.ds(0, 2), dr, :]))
        return moves

    def coarse_moves(ref, depth, tiles):
        moves = []
        for i, j, k in DIAGONAL_FIRST:
            (sp, dp), (sr, dr) = halo(i, P1, 4, depth), halo(j, W1, 4, depth)
            if tiles:
                moves.append(((i, j, k), ref.at[sp, :, sr, :], ref.at[dp, :, dr, :]))
            else:
                moves.append(((i, j, k), ref.at[sp, sr, :], ref.at[dp, dr, :]))
        return moves

    loads = []
    for a, source in enumerate((b_ref, k_ref)):
        for tile in range(2):
            loads.append(
                pltpu.make_async_copy(
                    source.at[:, :, pl.ds(128 * tile, 128)],
                    ext.at[a, pl.ds(P0, 8), tile, pl.ds(W0, 8), :],
                    load.at[2 * a + tile],
                )
            )
            loads[-1].start()
    barrier = pltpu.get_barrier_semaphore()

    def greet(ok, i, j, k):
        @pl.when(ok)
        def _():
            pl.semaphore_signal(barrier, inc=1, device_id=(i, j, k), device_id_type=MESH)

        return jnp.where(ok, 1, 0)

    count = 0
    for j in range(-REACH, REACH + 1):
        if abs(j) < ny:
            for gx in range(nx):
                count = count + greet(gx != mx if j == 0 else inside(0, j, 0), gx, my + j, mz)
    for i, j, k in STACK:
        count = count + greet(inside(i, j, k), mx + i, my + j, mz + k)
    for copy in loads:
        copy.wait()
    zero(tmp)
    zero(tmp2)
    pack_edges([lambda i, t: ext[0, P0 + i, t, W0 : W0 + 8, :], lambda i, t: ext[1, P0 + i, t, W0 : W0 + 8, :]], edge_out)
    with jax.named_scope("barrier"):
        pl.semaphore_wait(barrier, count)
    moves = edge_moves(edge_out, edge_in, 8)
    for (offset, src_b, dst_b), (_, src_k, dst_k) in zip(fine_moves(ext.at[0], 4), fine_moves(ext.at[1], 5)):
        moves += [(offset, src_b, dst_b), (offset, src_k, dst_k)]
    x0_arrive, x0_left = exchange(moves, 144, 82, 8)

    for ref in (redge_in, rext, bin1, bedge_in, dia1, rex1, xex1):
        zero(ref)
    own_k1 = coarse_of(lambda i, parity, t: ext[1, P0 + i, t, pl.ds(W0 + parity, 4, stride=2), :], 4, 4)
    for i, value in enumerate(own_k1):
        kin1[P1 + i, W1 : W1 + 4, :] = value
    pack_coarse(kedge_out)
    k1_arrive, k1_left = exchange(edge_moves(kedge_out, kedge_in, 4) + coarse_moves(kin1, 4, False), 16, 16, 4)
    for ref in (va0, wa0, vb0, wb0, va1, wa1, vb1, wb1, kap2, va2, wa2, vb2, wb2, xs2):
        zero(ref)
    x0_arrive()

    def put(a):
        def write(p, value):
            ext[a, p, 2] = value

        return write

    unpack_edges(edge_in, 0, put(0))
    unpack_edges(edge_in, 1, put(1))
    row = lax.broadcasted_iota(jnp.int32, (24, 128), 0)

    def planes_in(p, own, width):
        return (mx > 0) if p < own else ((mx < nx - 1) if p >= own + width else None)

    def inside_rows(p, own, width, own_row, width_row, depth):
        start = jnp.where(my > 0, own_row - depth, own_row)
        stop = jnp.where(my < ny - 1, own_row + width_row + depth, own_row + width_row)
        ok = planes_in(p, own, width)
        if ok is not None:
            stop = jnp.where(ok, stop, 0)
        return (row >= start) & (row < stop)

    for p in range(18):
        mask = inside_rows(p, P0, 8, W0, 8, 5)
        for tile in range(3):
            kap0[p, tile] = jnp.where(mask, ext[1, p, tile] * (0.5 / 30.0), 0.0)
    theta0, weights0 = chebyshev_coefs(DEGREE, FINE_LOW)
    lo, hi = P0 - 4, P0 + 12

    def start_level(level, planes, row, rows, theta, r_in, r_out, v_ref, w_ref, make_diagonal, size=2):
        kappa, diagonal, inverse = level
        for first, n in chunks(planes[0], planes[1], size):
            at = (pl.ds(first, n), slice(None), pl.ds(row, rows), slice(None))
            kap = kappa[at]
            if make_diagonal:
                dia = 128.0 * kap + stencil_sum(kappa, first, n, row, rows)
                diagonal[at] = dia
            else:
                dia = diagonal[at]
            inv = jnp.where(kap > 0.0, 1.0 / dia, 0.0)
            inverse[at] = inv
            r = jnp.where(kap > 0.0, r_in(at), 0.0)
            r_out[at] = r
            new = (theta * inv) * r
            v_ref[at] = new
            w_ref[at] = kap * new

    level0 = (kap0, dia0, inv0)
    start_level(level0, (lo, hi), 4, 16, theta0, lambda at: ext[(0,) + at], res0, va0, wa0, True)

    def own0(ref):
        return ref[P0 : P0 + 8, 0:2, W0 : W0 + 8, :]

    def put_res0(first, n, r):
        res0[pl.ds(first, n), :, 4:20, :] = r

    xs0[...] = own0(va0)
    here, there = (va0, wa0), (vb0, wb0)

    def smooth0(step, r_in):
        nonlocal here, there
        apply(level0, here, r_in, put_res0, (P0 - 3 + step, P0 + 11 - step), 4, 16, weights0[step], there)
        xs0[...] += own0(there[0])
        here, there = there, here

    smooth0(0, lambda at: res0[at])
    smooth0(1, lambda at: res0[at])

    k1_arrive()
    for p in range(12):
        mask = inside_rows(p, P1, 4, W1, 4, 4)
        kap1[p, 0] = jnp.where(mask, kin1[p] * (0.125 / 30.0), 0.0)
        kap1[p, 1] = jnp.where(mask, unpack_coarse(kedge_in, p) * (0.125 / 30.0), 0.0)
    for first, n in chunks(P1, P1 + 4, 2):
        at = (pl.ds(first, n), slice(None), pl.ds(W1, 8), slice(None))
        value = 128.0 * kap1[at] + stencil_sum(kap1, first, n, W1, 8)
        dia1[first : first + n, :, W1 : W1 + 4, :] = value[:, :, 0:4]
    d1_arrive, d1_left = exchange(coarse_moves(dia1, 4, True), 32, 32, 0)
    own_k2 = coarse_of(lambda i, parity, t: kap1[P1 + i, t, pl.ds(W1 + parity, 2, stride=2), :], 2, 2)
    for i, value in enumerate(own_k2):
        kin2[P2 + 2 * mx + i, 0, W2 : W2 + 2, :] = 0.25 * value
    k2_arrive, k2_left = column_gather(kin2)
    smooth0(2, lambda at: res0[at])

    def put_rext(first, n, r):
        rext[0, pl.ds(first, n), 0:2, W0 : W0 + 8, :] = r[:, 0:2]

    apply(level0, here, lambda at: res0[at], put_rext, (P0, P0 + 8), W0, 8, None)

    own_b1 = coarse_of(lambda i, parity, t: rext[0, P0 + i, t, pl.ds(W0 + parity, 4, stride=2), :], 4, 4)
    for i, value in enumerate(own_b1):
        bin1[P1 + i, W1 : W1 + 4, :] = value
    pack_coarse(bedge_out)
    b1_arrive, b1_left = exchange(edge_moves(bedge_out, bedge_in, 4) + coarse_moves(bin1, 4, False), 16, 16, 4)
    pack_edges([lambda i, t: rext[0, P0 + i, t, W0 : W0 + 8, :]], redge_out)
    x0_left()
    k1_left()
    d1_arrive()
    d1_left()
    b1_arrive()
    for p in range(12):
        res1[p, 0] = bin1[p]
        res1[p, 1] = unpack_coarse(bedge_in, p)
    level1 = (kap1, dia1, inv1)
    start_level(level1, (0, 12), 4, 16, theta0, lambda at: res1[at], res1, va1, wa1, False)

    def own1(ref):
        return ref[P1 : P1 + 4, :, W1 : W1 + 8, :]

    def put_res1(first, n, r):
        res1[pl.ds(first, n), :, 4:20, :] = r

    xs1[...] = own1(va1)
    here, there = (va1, wa1), (vb1, wb1)
    for step in range(3):
        apply(level1, here, lambda at: res1[at], put_res1, (P1 - 3 + step, P1 + 7 - step), 4, 16, weights0[step], there)
        xs1[...] += own1(there[0])
        here, there = there, here

    def put_rex1(first, n, r):
        rex1[pl.ds(first, n), :, W1 : W1 + 4, :] = r[:, :, 0:4]

    apply(level1, here, lambda at: res1[at], put_rex1, (P1, P1 + 4), W1, 8, None)

    own_b2 = coarse_of(lambda i, parity, t: rex1[P1 + i, t, pl.ds(W1 + parity, 2, stride=2), :], 2, 2)
    for i, value in enumerate(own_b2):
        bin2[P2 + 2 * mx + i, 0, W2 : W2 + 2, :] = value
    b2_arrive, b2_left = plane_gather(bin2)
    r1_arrive, r1_left = exchange(coarse_moves(rex1, 3, True), 24, 18, 0)
    k2_arrive()
    m2_arrive, m2_left = row_gather(kin2)
    k2_left()
    b1_left()
    m2_arrive()
    m2_left()
    full = 2 * nx
    at_row = lax.broadcasted_iota(jnp.int32, (full, 1, 24, 128), 2) + (8 - W2)
    start, stop = jnp.maximum(-2 * REACH, -2 * my), jnp.minimum(2 * REACH + 2, 2 * (ny - my))
    window = (slice(P2, P2 + full), slice(None), slice(8, 32), slice(None))
    kap2[window] = jnp.where((at_row >= start) & (at_row < stop), kin2[window], 0.0)
    theta2, weights2 = chebyshev_coefs(COARSE_DEGREE, COARSE_LOW)
    level2 = (kap2, dia2, inv2)
    b2_arrive()
    r0_arrive, r0_left = exchange(edge_moves(redge_out, redge_in, 8) + fine_moves(rext.at[0], 4), 64, 32, 8)
    start_level(level2, (P2, P2 + full), 8, 24, theta2, lambda at: bin2[at], res2, va2, wa2, True)
    xs2[window] = va2[window]
    here, there = (va2, wa2), (vb2, wb2)

    def put_res2(first, n, r):
        res2[pl.ds(first, n), :, 8:32, :] = r

    for step in range(COARSE_DEGREE - 1):
        apply(level2, here, lambda at: res2[at], put_res2, (P2, P2 + full), 8, 24, weights2[step], there)
        xs2[window] += there[0][window]
        here, there = there, here

    half = lanes_of((8, 128)) // 2
    for j in range(6):
        coarse = xs2[P2 + 2 * mx - 2 + j, 0, W2 - 2 : W2 + 6, :]
        for tile in range(2):
            value = pair_gather(coarse, half + 64 * tile)[0:6]
            for e in range(2):
                for parity in range(2):
                    va1[2 * j + e, tile, pl.ds(W1 - 4 + parity, 6, stride=2), :] = value
    for first, n in chunks(0, 12, 2):
        wa1[first : first + n] = kap1[first : first + n] * va1[first : first + n]
    xs1[...] += own1(va1)
    r1_arrive()
    here, there = (va1, wa1), (vb1, wb1)
    apply(level1, here, lambda at: rex1[at], put_res1, (P1 - 3, P1 + 7), 4, 16, (None, theta0), there)
    xs1[...] += own1(there[0])
    here, there = there, here
    for step in range(3):
        apply(level1, here, lambda at: res1[at], put_res1, (P1 - 2 + step, P1 + 6 - step), 4, 16, weights0[step], there)
        xs1[...] += own1(there[0])
        here, there = there, here
    xex1[P1 : P1 + 4, :, W1 : W1 + 4, :] = xs1[:, :, 0:4, :]
    x1_arrive, x1_left = exchange(coarse_moves(xex1, 3, True), 24, 18, 0)
    b2_left()
    r1_left()
    r0_left()
    r0_arrive()

    def put_rext2(p, value):
        rext[0, p, 2] = value

    unpack_edges(redge_in, 0, put_rext2)
    x1_arrive()
    lane = lanes_of((8, 128))
    ends = jnp.where(lane < 64, half, half + 64)
    for p in range(1, 11):
        for source_row, keep in ((W1 - 4, 8), (W1 + 4, 4)):
            for tile, source_tile, index in ((0, 0, half), (1, 0, half + 64), (2, 1, ends)):
                value = pair_gather(xex1[p, source_tile, source_row : source_row + 8, :], index)[0:keep]
                for q in (2 * p - 3, 2 * p - 2):
                    if 0 <= q < 18:
                        for parity in range(2):
                            va0[q, tile, pl.ds(2 * (source_row - 4) + parity, keep, stride=2), :] = value
    for first, n in chunks(0, 18, 2):
        wa0[first : first + n] = kap0[first : first + n] * va0[first : first + n]
    xs0[...] += own0(va0)
    here, there = (va0, wa0), (vb0, wb0)
    apply(level0, here, lambda at: rext[(0,) + at], put_res0, (lo, hi), 4, 16, (None, theta0), there)
    xs0[...] += own0(there[0])
    here, there = there, here
    for step in range(3):
        smooth0(step, lambda at: res0[at])

    def put_out(first, n, r):
        for tile in range(2):
            r_ref[first - P0 : first - P0 + n, :, 128 * tile : 128 * tile + 128] = r[:, tile]

    apply(level0, here, lambda at: res0[at], put_out, (P0, P0 + 8), W0, 8, None)
    for tile in range(2):
        x_ref[:, :, 128 * tile : 128 * tile + 128] = xs0[:, tile]
    x1_left()


def solution(mesh):
    sizes = tuple(mesh.shape[axis] for axis in ("gx", "gy", "gz"))

    def step(conductivity, source):
        def vmem(*shape):
            return pltpu.VMEM(shape, F32)

        level0, level1, level2 = (18, 3, 24, 128), (12, 2, 24, 128), (12, 1, 40, 128)
        sems = 10
        shape = jax.ShapeDtypeStruct(conductivity.shape, F32)
        return pl.pallas_call(
            lambda *refs: kernel(sizes, *refs),
            name="cycle",
            out_shape=(shape, shape),
            in_specs=[pl.BlockSpec(memory_space=pltpu.HBM)] * 2,
            out_specs=(pl.BlockSpec(memory_space=pltpu.VMEM),) * 2,
            scratch_shapes=[
                vmem(2, *level0), vmem(2, 3, 24, 128), vmem(2, 8, 128), vmem(2, 3, 24, 128), vmem(2, 8, 128), vmem(1, *level0),
                *[vmem(*level0) for _ in range(8)], vmem(8, 2, 8, 128),
                vmem(12, 24, 128), vmem(12, 24, 128), *[vmem(*s) for s in 2 * ((2, 3, 24, 128), (2, 8, 128))], *[vmem(*level1) for _ in range(10)], vmem(4, 2, 8, 128),
                *[vmem(*level2) for _ in range(11)],
                vmem(2, 16, 128), vmem(24, 128), vmem(1152, 128),
                pltpu.SemaphoreType.DMA((sems,)), pltpu.SemaphoreType.DMA((sems,)), pltpu.SemaphoreType.DMA((4,)),
            ],
            compiler_params=pltpu.CompilerParams(
                collective_id=0, has_side_effects=True, vmem_limit_bytes=50 * 1024 * 1024
            ),
        )(*(pltpu.with_memory_space_constraint(v, pltpu.HBM) for v in (conductivity, source)))

    spec = P("gx", "gy", "gz")
    return jax.shard_map(step, mesh=mesh, in_specs=(spec, spec), out_specs=(spec, spec), check_vma=False)
```

```python
import jax
import jax.numpy as jnp
from jax import lax
from jax.experimental import pallas as pl
from jax.experimental.pallas import tpu as pltpu
from jax.sharding import PartitionSpec as P

MESH = pl.DeviceIdType.MESH
F32 = jnp.float32
DEGREE = 4
COARSE_DEGREE = 8
UPPER = 2.0
FINE_LOW = 0.5
COARSE_LOW = 0.03
REACH = 5

P0, W0 = 5, 8
P1, W1 = 4, 8
P2, W2 = 2, 18
SIDES = (-1, 0, 1)
FINE = 7
FLAT = [(i, j, 0) for i in SIDES for j in SIDES if (i, j) != (0, 0)]
STACK = [(i, j, k) for k in (-1, 1) for i in SIDES for j in SIDES]
NEXT, OVER = [(0, -1, 0), (0, 1, 0)], [(0, -2, 0), (0, 2, 0)]
DIAGONAL_FIRST = sorted(FLAT, key=lambda o: -abs(o[0]) - abs(o[1]))


def chebyshev_coefs(degree, lower):
    centre = (UPPER + lower) / 2.0
    half_width = (UPPER - lower) / 2.0
    ratio_term = centre / half_width
    rho_prev = 1.0 / ratio_term
    weights = []
    for _ in range(1, degree):
        rho_next = 1.0 / (2.0 * ratio_term - rho_prev)
        weights.append((rho_next * rho_prev, 2.0 * rho_next / half_width))
        rho_prev = rho_next
    return 1.0 / centre, weights


def rolled(values, shift):
    flat = values.reshape(-1, 128)
    return pltpu.roll(flat, shift % 128, 1).reshape(values.shape)


def lanes_of(shape):
    return lax.broadcasted_iota(jnp.int32, shape, len(shape) - 1)


def beside(values):
    up, down = rolled(values, 1), rolled(values, -1)
    tiles = values.shape[1]
    if tiles > 1:
        lane = lanes_of(values.shape)
        before = jnp.concatenate([up[:, tiles - 1 :], up[:, : tiles - 1]], axis=1)
        after = jnp.concatenate([down[:, 1:], down[:, :1]], axis=1)
        up = jnp.where(lane == 0, before, up)
        down = jnp.where(lane == 127, after, down)
    return up + down


def stencil_sum(ref, first, count, row, rows):
    planes = pl.ds(first - 1, count + 2)
    centre = ref[planes, :, pl.ds(row, rows), :]
    side = ref[planes, :, pl.ds(row - 1, rows), :] + ref[planes, :, pl.ds(row + 1, rows), :]
    corner = 3.0 * centre + side
    face = 14.0 * centre + 3.0 * side
    outer = face[1:-1] + corner[:-2] + corner[2:]
    middle = 14.0 * side[1:-1] + face[:-2] + face[2:]
    return middle + beside(outer)


def chunks(first, last, size):
    return [(at, min(size, last - at)) for at in range(first, last, size)]


def apply(level, source, r_in, r_out, planes, row, rows, coefs, target=None, size=2):
    kappa, diagonal, inverse = level
    v_ref, w_ref = source
    for first, count in chunks(planes[0], planes[1], size):
        at = (pl.ds(first, count), slice(None), pl.ds(row, rows), slice(None))
        v = v_ref[at]
        r = r_in(at) - diagonal[at] * v
        r = r + kappa[at] * stencil_sum(v_ref, first, count, row, rows)
        r = r + stencil_sum(w_ref, first, count, row, rows)
        if callable(r_out):
            r_out(first, count, r)
        else:
            r_out[at] = r
        if coefs is not None:
            new = (coefs[1] * inverse[at]) * r
            if coefs[0] is not None:
                new = new + coefs[0] * v
            target[0][at] = new
            target[1][at] = kappa[at] * new


def pair_gather(values, index):
    return jnp.take_along_axis(values, index, axis=1)


def kernel(sizes, k_ref, b_ref, x_ref, r_ref, ext, edge_in, edge_out, redge_in, redge_out, rext,
           kap0, dia0, inv0, res0, va0, wa0, vb0, wb0, xs0,
           kin1, bin1, kedge_in, kedge_out, bedge_in, bedge_out, kap1, dia1, inv1, res1, va1, wa1, vb1, wb1, rex1, xex1, xs1,
           kin2, kap2, dia2, inv2, bin2, res2, va2, wa2, vb2, wb2, xs2, tmp, tmp2, spare, send, recv, load, news):
    nx, ny, nz = sizes
    mx, my, mz = lax.axis_index("gx"), lax.axis_index("gy"), lax.axis_index("gz")
    used = [0]

    def inside(i, j, k):
        tests = []
        if i < 0:
            tests.append(mx + i >= 0)
        if i > 0:
            tests.append(mx + i < nx)
        if j < 0:
            tests.append(my + j >= 0)
        if j > 0:
            tests.append(my + j < ny)
        if k < 0:
            tests.append(mz + k >= 0)
        if k > 0:
            tests.append(mz + k < nz)
        ok = tests[0]
        for test in tests[1:]:
            ok = ok & test
        return ok

    def amount(where, rows, number, sent):
        whole = spare.at[pl.ds(0, rows)]

        @pl.when(where)
        def _():
            copy = pltpu.make_async_remote_copy(
                src_ref=whole, dst_ref=whole, send_sem=send.at[number], recv_sem=recv.at[number],
                device_id=(mx, my, mz), device_id_type=MESH,
            )
            if sent:
                copy.wait_send()
            else:
                copy.wait_recv()

    def waits(number, cases):
        def wait(sent):
            with jax.named_scope(f"{'sent' if sent else 'wait'}{number}"):
                for where, rows in cases:
                    amount(where, rows, number, sent)

        return (lambda: wait(False)), (lambda: wait(True))

    def some(n):
        return (1, 2) if n > 2 else (1,)

    near_x = jnp.where(mx > 0, 1, 0) + jnp.where(mx < nx - 1, 1, 0)
    near_y = jnp.where(my > 0, 1, 0) + jnp.where(my < ny - 1, 1, 0)
    near_z = jnp.where(mz > 0, 1, 0) + jnp.where(mz < nz - 1, 1, 0)
    low_y, high_y = jnp.minimum(my, REACH), jnp.minimum(ny - 1 - my, REACH)
    far_counts = sorted({min(y, REACH) + min(ny - 1 - y, REACH) for y in range(ny)})

    def exchange(moves, face, corner, stack):
        number = used[0]
        used[0] += 1
        for (i, j, k), src, dst in moves:
            copy = pltpu.make_async_remote_copy(
                src_ref=src, dst_ref=dst, send_sem=send.at[number], recv_sem=recv.at[number],
                device_id=(mx + i, my + j, mz + k), device_id_type=MESH,
            )
            pl.when(inside(i, j, k))(copy.start)
        cases = []
        for x in some(nx):
            for y in some(ny):
                for z in some(nz) if stack else (0,):
                    where = (near_x == x) & (near_y == y)
                    if stack:
                        where = where & (near_z == z)
                    cases.append((where, (x + y) * face + x * y * corner + (z * (1 + x) * (stack[0] + y * stack[1]) if stack else 0)))
        return waits(number, cases)

    def mine(ref):
        return ref.at[pl.ds(P2 + 2 * mx, 2), :, pl.ds(W2, 2), :]

    def far_start(ref, number, shift, j):
        copy = pltpu.make_async_remote_copy(
            src_ref=mine(ref), dst_ref=ref.at[pl.ds(P2 + 2 * mx, 2), :, pl.ds(W2 - 2 * j, 2), :],
            send_sem=send.at[number], recv_sem=recv.at[number],
            device_id=(lax.rem(mx + shift, nx), my + j, mz), device_id_type=MESH,
        )
        if j == 0:
            copy.start()
        else:
            pl.when(inside(0, j, 0))(copy.start)

    distances = [j for j in sorted(range(-REACH, REACH + 1), key=lambda o: -abs(o)) if abs(j) < ny]

    def column_gather(ref):
        number = used[0]
        used[0] += 1
        for j in distances:
            if j != 0:
                far_start(ref, number, 0, j)
        return waits(number, [(low_y + high_y == c, 4 * c) for c in far_counts])

    def plane_gather(ref):
        number = used[0]
        used[0] += 1
        for j in distances:
            for shift in range(nx):
                if (shift, j) != (0, 0):
                    far_start(ref, number, shift, j)
        return waits(number, [(low_y + high_y == c, 4 * ((1 + c) * nx - 1)) for c in far_counts])

    def row_gather(ref):
        number = used[0]
        used[0] += 1
        part = ref.at[pl.ds(P2 + 2 * mx, 2), :, pl.ds(W2 - 2 * REACH, 4 * REACH + 2), :]
        for shift in range(1, nx):
            pltpu.make_async_remote_copy(
                src_ref=part, dst_ref=part, send_sem=send.at[number], recv_sem=recv.at[number],
                device_id=(lax.rem(mx + shift, nx), my, mz), device_id_type=MESH,
            ).start()
        return waits(number, [(mx >= 0, (nx - 1) * 2 * (4 * REACH + 2))])

    def zero(ref):
        ref[...] = jnp.zeros(ref.shape, F32)

    def coarse_of(read, count, rows):
        for tile in range(2):
            for i in range(count):
                total = read(2 * i, 0, tile) + read(2 * i, 1, tile) + read(2 * i + 1, 0, tile) + read(2 * i + 1, 1, tile)
                tmp[tile, rows * i : rows * (i + 1), :] = 0.125 * total
        size = max(8, count * rows)
        lane = lanes_of((size, 128))
        pairs = [tmp[tile, 0:size, :] for tile in range(2)]
        pairs = [p + pltpu.roll(p, 127, 1) for p in pairs]
        index = (2 * lane) % 128
        out = jnp.where(lane < 64, pair_gather(pairs[0], index), pair_gather(pairs[1], index))
        tmp2[0:size, :] = out
        return [tmp2[rows * i : rows * (i + 1), :] for i in range(count)]

    def pack_edges(reads, out):
        for way, (tile, start) in enumerate(((1, 120), (0, 0))):
            packed = jnp.zeros((8, 128), F32)
            lane = lanes_of((8, 128))
            for a, read in enumerate(reads):
                for i in range(8):
                    at = 8 * i + 64 * a
                    part = pltpu.roll(read(i, tile), (at - start) % 128, 1)
                    packed = jnp.where((lane >= at) & (lane < at + 8), part, packed)
            out[way] = packed

    def edge_moves(src, dst, own, width, depth):
        moves = []
        for i, j, k in STACK:
            way, side = (0, 0) if k > 0 else (1, 1)
            rows, there = halo(j, own, width, depth)
            mine_rows = pl.ds(rows.start - own, rows.size)
            moves.append(((i, j, k), src.at[way, mine_rows, :], dst.at[side, 1 - i, there, :]))
        return moves

    def pack_coarse(out):
        lane = lanes_of((4, 128))
        for way, start in enumerate((96, 0)):
            packed = jnp.zeros((4, 128), F32)
            for i in range(4):
                part = pltpu.roll(tmp2[4 * i : 4 * i + 8, :], (32 * i - start) % 128, 1)[0:4]
                packed = jnp.where((lane >= 32 * i) & (lane < 32 * i + 32), part, packed)
            out[way, 0:4] = packed

    def unpack_coarse(src, p):
        lane = lanes_of((24, 128))
        high_end, low_start = jnp.where(mz < nz - 1, 32, 0), jnp.where(mz > 0, 96, 128)
        low = pltpu.roll(src[0, p // 4], (96 - 32 * (p % 4)) % 128, 1)
        high = pltpu.roll(src[1, p // 4], (-32 * (p % 4)) % 128, 1)
        return jnp.where(lane < high_end, high, jnp.where(lane >= low_start, low, 0.0))

    def unpack_edges(src, a, write):
        lane = lanes_of((24, 128))
        high_end, low_start = jnp.where(mz < nz - 1, 8, 0), jnp.where(mz > 0, 120, 128)
        for p in range(2 * P0 + 8):
            group, i = (0, 3 + p) if p < P0 else ((1, p - P0) if p < P0 + 8 else (2, p - P0 - 8))
            at = 8 * i + 64 * a
            low = pltpu.roll(src[0, group], (120 - at) % 128, 1)
            high = pltpu.roll(src[1, group], -at % 128, 1)
            write(p, jnp.where(lane < high_end, high, jnp.where(lane >= low_start, low, 0.0)))

    def halo(step, own, width, depth):
        if step == 0:
            return pl.ds(own, width), pl.ds(own, width)
        if step > 0:
            return pl.ds(own + width - depth, depth), pl.ds(own - depth, depth)
        return pl.ds(own, depth), pl.ds(own + width, depth)

    def fine_moves(ref, depth):
        moves = []
        for i, j, k in DIAGONAL_FIRST:
            (sp, dp), (sr, dr) = halo(i, P0, 8, depth), halo(j, W0, 8, depth)
            moves.append(((i, j, k), ref.at[sp, pl.ds(0, 2), sr, :], ref.at[dp, pl.ds(0, 2), dr, :]))
        return moves

    def coarse_moves(ref, depth, tiles):
        moves = []
        for i, j, k in DIAGONAL_FIRST:
            (sp, dp), (sr, dr) = halo(i, P1, 4, depth), halo(j, W1, 4, depth)
            if tiles:
                moves.append(((i, j, k), ref.at[sp, :, sr, :], ref.at[dp, :, dr, :]))
            else:
                moves.append(((i, j, k), ref.at[sp, sr, :], ref.at[dp, dr, :]))
        return moves

    loads = []
    for a, source in enumerate((b_ref, k_ref)):
        for tile in range(2):
            loads.append(
                pltpu.make_async_copy(
                    source.at[:, :, pl.ds(128 * tile, 128)],
                    ext.at[a, pl.ds(P0, 8), tile, pl.ds(W0, 8), :],
                    load.at[2 * a + tile],
                )
            )
            loads[-1].start()
    barrier = pltpu.get_barrier_semaphore()

    def tell(offsets, semaphore):
        for i, j, k in offsets:

            @pl.when(inside(i, j, k))
            def _():
                pl.semaphore_signal(semaphore, inc=1, device_id=(mx + i, my + j, mz + k), device_id_type=MESH)

    def hear(offsets, semaphore):
        with jax.named_scope("hear"):
            pl.semaphore_wait(semaphore, sum(jnp.where(inside(i, j, k), 1, 0) for i, j, k in offsets))

    tell(STACK + FLAT, barrier)
    zero(tmp)
    zero(tmp2)
    for copy in loads:
        copy.wait()
    pack_edges([lambda i, t: ext[0, P0 + i, t, W0 : W0 + 8, :], lambda i, t: ext[1, P0 + i, t, W0 : W0 + 8, :]], edge_out)
    hear(STACK + FLAT, barrier)
    moves = edge_moves(edge_out, edge_in, W0, 8, 5)
    for (offset, src_b, dst_b), (_, src_k, dst_k) in zip(fine_moves(ext.at[0], 4), fine_moves(ext.at[1], 5)):
        moves += [(offset, src_b, dst_b), (offset, src_k, dst_k)]
    x0_arrive, x0_left = exchange(moves, 144, 82, (8, 5))

    tell(NEXT, news.at[0])

    for ref in (redge_in, rext, bin1, bedge_in, dia1, rex1, xex1):
        zero(ref)
    own_k1 = coarse_of(lambda i, parity, t: ext[1, P0 + i, t, pl.ds(W0 + parity, 4, stride=2), :], 4, 4)
    for i, value in enumerate(own_k1):
        kin1[P1 + i, W1 : W1 + 4, :] = value
    pack_coarse(kedge_out)
    k1_arrive, k1_left = exchange(edge_moves(kedge_out, kedge_in, W1, 4, 4) + coarse_moves(kin1, 4, False), 16, 16, (4, 4))
    for ref in (va0, wa0, vb0, wb0, va1, wa1, vb1, wb1, kap2, va2, wa2, vb2, wb2, xs2):
        zero(ref)
    hear(NEXT, news.at[0])
    tell(OVER, news.at[1])
    hear(OVER, news.at[1])
    tell(FLAT, news.at[2])
    x0_arrive()
    def put(a):
        def write(p, value):
            ext[a, p, 2] = value

        return write

    unpack_edges(edge_in, 0, put(0))
    unpack_edges(edge_in, 1, put(1))
    row = lax.broadcasted_iota(jnp.int32, (24, 128), 0)

    def planes_in(p, own, width):
        return (mx > 0) if p < own else ((mx < nx - 1) if p >= own + width else None)

    def inside_rows(p, own, width, own_row, width_row, depth):
        start = jnp.where(my > 0, own_row - depth, own_row)
        stop = jnp.where(my < ny - 1, own_row + width_row + depth, own_row + width_row)
        ok = planes_in(p, own, width)
        if ok is not None:
            stop = jnp.where(ok, stop, 0)
        return (row >= start) & (row < stop)

    for p in range(18):
        mask = inside_rows(p, P0, 8, W0, 8, 5)
        for tile in range(3):
            kap0[p, tile] = jnp.where(mask, ext[1, p, tile] * (0.5 / 30.0), 0.0)
    theta0, weights0 = chebyshev_coefs(DEGREE, FINE_LOW)
    lo, hi = P0 - 4, P0 + 12

    def start_level(level, planes, row, rows, theta, r_in, r_out, v_ref, w_ref, make_diagonal, size=2):
        kappa, diagonal, inverse = level
        for first, n in chunks(planes[0], planes[1], size):
            at = (pl.ds(first, n), slice(None), pl.ds(row, rows), slice(None))
            kap = kappa[at]
            if make_diagonal:
                dia = 128.0 * kap + stencil_sum(kappa, first, n, row, rows)
                diagonal[at] = dia
            else:
                dia = diagonal[at]
            inv = jnp.where(kap > 0.0, 1.0 / dia, 0.0)
            inverse[at] = inv
            r = jnp.where(kap > 0.0, r_in(at), 0.0)
            r_out[at] = r
            new = (theta * inv) * r
            v_ref[at] = new
            w_ref[at] = kap * new

    level0 = (kap0, dia0, inv0)
    start_level(level0, (lo, hi), 4, 16, theta0, lambda at: ext[(0,) + at], res0, va0, wa0, True, FINE)

    def own0(ref):
        return ref[P0 : P0 + 8, 0:2, W0 : W0 + 8, :]

    xs0[...] = own0(va0)
    here, there = (va0, wa0), (vb0, wb0)

    def smooth0(step, r_in):
        nonlocal here, there
        apply(level0, here, r_in, res0, (P0 - 3 + step, P0 + 11 - step), 4, 16, weights0[step], there, FINE)
        xs0[...] += own0(there[0])
        here, there = there, here

    smooth0(0, lambda at: res0[at])
    smooth0(1, lambda at: res0[at])

    k1_arrive()
    for p in range(12):
        mask = inside_rows(p, P1, 4, W1, 4, 4)
        kap1[p, 0] = jnp.where(mask, kin1[p] * (0.125 / 30.0), 0.0)
        kap1[p, 1] = jnp.where(mask, unpack_coarse(kedge_in, p) * (0.125 / 30.0), 0.0)
    for first, n in chunks(P1, P1 + 4, 2):
        at = (pl.ds(first, n), slice(None), pl.ds(W1, 8), slice(None))
        value = 128.0 * kap1[at] + stencil_sum(kap1, first, n, W1, 8)
        dia1[first : first + n, :, W1 : W1 + 4, :] = value[:, :, 0:4]
    hear(FLAT, news.at[2])
    d1_arrive, d1_left = exchange(coarse_moves(dia1, 4, True), 32, 32, None)
    smooth0(2, lambda at: res0[at])

    def put_rext(first, n, r):
        rext[0, pl.ds(first, n), 0:2, W0 : W0 + 8, :] = r[:, 0:2]

    apply(level0, here, lambda at: res0[at], put_rext, (P0, P0 + 8), W0, 8, None, None, FINE)

    own_b1 = coarse_of(lambda i, parity, t: rext[0, P0 + i, t, pl.ds(W0 + parity, 4, stride=2), :], 4, 4)
    for i, value in enumerate(own_b1):
        bin1[P1 + i, W1 : W1 + 4, :] = value
    pack_coarse(bedge_out)
    b1_arrive, b1_left = exchange(edge_moves(bedge_out, bedge_in, W1, 4, 4) + coarse_moves(bin1, 4, False), 16, 16, (4, 4))
    own_k2 = coarse_of(lambda i, parity, t: kap1[P1 + i, t, pl.ds(W1 + parity, 2, stride=2), :], 2, 2)
    for i, value in enumerate(own_k2):
        kin2[P2 + 2 * mx + i, 0, W2 : W2 + 2, :] = 0.25 * value
    k2_arrive, k2_left = column_gather(kin2)
    pack_edges([lambda i, t: rext[0, P0 + i, t, W0 : W0 + 8, :]], redge_out)
    x0_left()
    k1_left()
    d1_arrive()
    d1_left()
    b1_arrive()
    r0_arrive, r0_left = exchange(edge_moves(redge_out, redge_in, W0, 8, 4) + fine_moves(rext.at[0], 4), 64, 32, (8, 4))
    for p in range(12):
        res1[p, 0] = bin1[p]
        res1[p, 1] = unpack_coarse(bedge_in, p)
    level1 = (kap1, dia1, inv1)
    start_level(level1, (0, 12), 4, 16, theta0, lambda at: res1[at], res1, va1, wa1, False)

    def own1(ref):
        return ref[P1 : P1 + 4, :, W1 : W1 + 8, :]

    xs1[...] = own1(va1)
    here, there = (va1, wa1), (vb1, wb1)
    for step in range(3):
        at_row, rows = ((4, 16), (6, 8), (7, 8))[step]
        apply(level1, here, lambda at: res1[at], res1, (P1 - 3 + step, P1 + 7 - step), at_row, rows, weights0[step], there)
        xs1[...] += own1(there[0])
        here, there = there, here

    def put_rex1(first, n, r):
        rex1[pl.ds(first, n), :, W1 : W1 + 4, :] = r[:, :, 0:4]

    apply(level1, here, lambda at: res1[at], put_rex1, (P1, P1 + 4), W1, 8, None)

    own_b2 = coarse_of(lambda i, parity, t: rex1[P1 + i, t, pl.ds(W1 + parity, 2, stride=2), :], 2, 2)
    for i, value in enumerate(own_b2):
        bin2[P2 + 2 * mx + i, 0, W2 : W2 + 2, :] = value
    b2_arrive, b2_left = plane_gather(bin2)
    k2_arrive()
    m2_arrive, m2_left = row_gather(kin2)
    r1_arrive, r1_left = exchange(coarse_moves(rex1, 3, True), 24, 18, None)
    k2_left()
    b1_left()
    m2_arrive()
    m2_left()
    full = 2 * nx
    at_row = lax.broadcasted_iota(jnp.int32, (full, 1, 24, 128), 2) + (8 - W2)
    start, stop = jnp.maximum(-2 * REACH, -2 * my), jnp.minimum(2 * REACH + 2, 2 * (ny - my))
    window = (slice(P2, P2 + full), slice(None), slice(8, 32), slice(None))
    kap2[window] = jnp.where((at_row >= start) & (at_row < stop), kin2[window], 0.0)
    theta2, weights2 = chebyshev_coefs(COARSE_DEGREE, COARSE_LOW)
    level2 = (kap2, dia2, inv2)
    b2_arrive()
    start_level(level2, (P2, P2 + full), 8, 24, theta2, lambda at: bin2[at], res2, va2, wa2, True)
    near = (slice(P2, P2 + full), slice(None), slice(W2 - 3, W2 + 5), slice(None))
    xs2[near] = va2[near]
    here, there = (va2, wa2), (vb2, wb2)
    for step in range(COARSE_DEGREE - 1):
        at_row, rows = (8, 24) if step == 0 else ((W2 - 7, 16) if step < 5 else (W2 - 3, 8))
        apply(level2, here, lambda at: res2[at], res2, (P2, P2 + full), at_row, rows, weights2[step], there)
        xs2[near] += there[0][near]
        here, there = there, here

    half = lanes_of((8, 128)) // 2
    for j in range(6):
        coarse = xs2[P2 + 2 * mx - 2 + j, 0, W2 - 2 : W2 + 6, :]
        for tile in range(2):
            value = pair_gather(coarse, half + 64 * tile)[0:6]
            for e in range(2):
                for parity in range(2):
                    va1[2 * j + e, tile, pl.ds(W1 - 4 + parity, 6, stride=2), :] = value
    for first, n in chunks(0, 12, 2):
        wa1[first : first + n] = kap1[first : first + n] * va1[first : first + n]
    xs1[...] += own1(va1)
    r1_arrive()
    here, there = (va1, wa1), (vb1, wb1)
    apply(level1, here, lambda at: rex1[at], res1, (P1 - 3, P1 + 7), 4, 16, (None, theta0), there)
    xs1[...] += own1(there[0])
    here, there = there, here
    for step in range(3):
        at_row = (6, 7, 8)[step]
        apply(level1, here, lambda at: res1[at], res1, (P1 - 2 + step, P1 + 6 - step), at_row, 8, weights0[step], there)
        xs1[...] += own1(there[0])
        here, there = there, here
    xex1[P1 : P1 + 4, :, W1 : W1 + 4, :] = xs1[:, :, 0:4, :]
    x1_arrive, x1_left = exchange(coarse_moves(xex1, 3, True), 24, 18, None)
    b2_left()
    r1_left()
    r0_left()
    r0_arrive()

    def put_rext2(p, value):
        rext[0, p, 2] = value

    unpack_edges(redge_in, 0, put_rext2)
    x1_arrive()
    lane = lanes_of((8, 128))
    ends = jnp.where(lane < 64, half, half + 64)
    for p in range(1, 11):
        for source_row, keep in ((W1 - 4, 8), (W1 + 4, 4)):
            for tile, source_tile, index in ((0, 0, half), (1, 0, half + 64), (2, 1, ends)):
                value = pair_gather(xex1[p, source_tile, source_row : source_row + 8, :], index)[0:keep]
                for q in (2 * p - 3, 2 * p - 2):
                    if 0 <= q < 18:
                        for parity in range(2):
                            va0[q, tile, pl.ds(2 * (source_row - 4) + parity, keep, stride=2), :] = value
    for first, n in chunks(0, 18, 2):
        wa0[first : first + n] = kap0[first : first + n] * va0[first : first + n]
    xs0[...] += own0(va0)
    here, there = (va0, wa0), (vb0, wb0)
    apply(level0, here, lambda at: rext[(0,) + at], res0, (lo, hi), 4, 16, (None, theta0), there, FINE)
    xs0[...] += own0(there[0])
    here, there = there, here
    for step in range(3):
        smooth0(step, lambda at: res0[at])

    def put_out(first, n, r):
        for tile in range(2):
            r_ref[first - P0 : first - P0 + n, :, 128 * tile : 128 * tile + 128] = r[:, tile]

    apply(level0, here, lambda at: res0[at], put_out, (P0, P0 + 8), W0, 8, None, None, FINE)
    for tile in range(2):
        x_ref[:, :, 128 * tile : 128 * tile + 128] = xs0[:, tile]
    x1_left()


def solution(mesh):
    sizes = tuple(mesh.shape[axis] for axis in ("gx", "gy", "gz"))

    def step(conductivity, source):
        def vmem(*shape):
            return pltpu.VMEM(shape, F32)

        level0, level1, level2 = (18, 3, 24, 128), (12, 2, 24, 128), (12, 1, 40, 128)
        sems = 10
        shape = jax.ShapeDtypeStruct(conductivity.shape, F32)
        return pl.pallas_call(
            lambda *refs: kernel(sizes, *refs),
            name="cycle",
            out_shape=(shape, shape),
            in_specs=[pl.BlockSpec(memory_space=pltpu.HBM)] * 2,
            out_specs=(pl.BlockSpec(memory_space=pltpu.VMEM),) * 2,
            scratch_shapes=[
                vmem(2, *level0), vmem(2, 3, 24, 128), vmem(2, 8, 128), vmem(2, 3, 24, 128), vmem(2, 8, 128), vmem(1, *level0),
                *[vmem(*level0) for _ in range(8)], vmem(8, 2, 8, 128),
                vmem(12, 24, 128), vmem(12, 24, 128), *[vmem(*s) for s in 2 * ((2, 3, 24, 128), (2, 8, 128))], *[vmem(*level1) for _ in range(10)], vmem(4, 2, 8, 128),
                *[vmem(*level2) for _ in range(11)],
                vmem(2, 16, 128), vmem(24, 128), vmem(1152, 128),
                pltpu.SemaphoreType.DMA((sems,)), pltpu.SemaphoreType.DMA((sems,)), pltpu.SemaphoreType.DMA((4,)),
                pltpu.SemaphoreType.REGULAR((3,)),
            ],
            compiler_params=pltpu.CompilerParams(
                collective_id=0, has_side_effects=True, vmem_limit_bytes=50 * 1024 * 1024
            ),
        )(*(pltpu.with_memory_space_constraint(v, pltpu.HBM) for v in (conductivity, source)))

    spec = P("gx", "gy", "gz")
    return jax.shard_map(step, mesh=mesh, in_specs=(spec, spec), out_specs=(spec, spec), check_vma=False)
```

```python
import jax
import jax.numpy as jnp
from jax import lax
from jax.experimental import pallas as pl
from jax.experimental.pallas import tpu as pltpu
from jax.sharding import PartitionSpec as P

MESH = pl.DeviceIdType.MESH
F32 = jnp.float32
DEGREE = 4
COARSE_DEGREE = 8
UPPER = 2.0
FINE_LOW = 0.5
COARSE_LOW = 0.03
REACH = 5

P0, W0 = 5, 8
P1, W1 = 4, 8
P2, W2 = 2, 18
SIDES = (-1, 0, 1)
FINE = 7
FLAT = [(i, j, 0) for i in SIDES for j in SIDES if (i, j) != (0, 0)]
STACK = [(i, j, k) for k in (-1, 1) for i in SIDES for j in SIDES]
NEXT, OVER = [(0, -1, 0), (0, 1, 0)], [(0, -2, 0), (0, 2, 0)]
DIAGONAL_FIRST = sorted(FLAT, key=lambda o: -abs(o[0]) - abs(o[1]))


def chebyshev_coefs(degree, lower):
    centre = (UPPER + lower) / 2.0
    half_width = (UPPER - lower) / 2.0
    ratio_term = centre / half_width
    rho_prev = 1.0 / ratio_term
    weights = []
    for _ in range(1, degree):
        rho_next = 1.0 / (2.0 * ratio_term - rho_prev)
        weights.append((rho_next * rho_prev, 2.0 * rho_next / half_width))
        rho_prev = rho_next
    return 1.0 / centre, weights


def rolled(values, shift):
    flat = values.reshape(-1, 128)
    return pltpu.roll(flat, shift % 128, 1).reshape(values.shape)


def lanes_of(shape):
    return lax.broadcasted_iota(jnp.int32, shape, len(shape) - 1)


def beside(values):
    up, down = rolled(values, 1), rolled(values, -1)
    tiles = values.shape[1]
    if tiles > 1:
        lane = lanes_of(values.shape)
        before = jnp.concatenate([up[:, tiles - 1 :], up[:, : tiles - 1]], axis=1)
        after = jnp.concatenate([down[:, 1:], down[:, :1]], axis=1)
        up = jnp.where(lane == 0, before, up)
        down = jnp.where(lane == 127, after, down)
    return up + down


def stencil_sum(ref, first, count, row, rows):
    planes = pl.ds(first - 1, count + 2)
    centre = ref[planes, :, pl.ds(row, rows), :]
    side = ref[planes, :, pl.ds(row - 1, rows), :] + ref[planes, :, pl.ds(row + 1, rows), :]
    corner = 3.0 * centre + side
    face = 14.0 * centre + 3.0 * side
    outer = face[1:-1] + corner[:-2] + corner[2:]
    middle = 14.0 * side[1:-1] + face[:-2] + face[2:]
    return middle + beside(outer)


def chunks(first, last, size):
    return [(at, min(size, last - at)) for at in range(first, last, size)]


def apply(level, source, r_in, r_out, planes, row, rows, coefs, target=None, size=2):
    kappa, diagonal, inverse = level
    v_ref, w_ref = source
    for first, count in chunks(planes[0], planes[1], size):
        at = (pl.ds(first, count), slice(None), pl.ds(row, rows), slice(None))
        v = v_ref[at]
        r = r_in(at) - diagonal[at] * v
        r = r + kappa[at] * stencil_sum(v_ref, first, count, row, rows)
        r = r + stencil_sum(w_ref, first, count, row, rows)
        if callable(r_out):
            r_out(first, count, r)
        else:
            r_out[at] = r
        if coefs is not None:
            new = (coefs[1] * inverse[at]) * r
            if coefs[0] is not None:
                new = new + coefs[0] * v
            target[0][at] = new
            target[1][at] = kappa[at] * new


def pair_gather(values, index):
    return jnp.take_along_axis(values, index, axis=1)


def kernel(sizes, k_ref, b_ref, x_ref, r_ref, ext, edge_in, edge_out, redge_in, redge_out, rext,
           kap0, dia0, inv0, res0, va0, wa0, vb0, wb0, xs0,
           kin1, bin1, kedge_in, kedge_out, bedge_in, bedge_out, kap1, dia1, inv1, res1, va1, wa1, vb1, wb1, rex1, xex1, xs1,
           kin2, kap2, dia2, inv2, bin2, res2, va2, wa2, vb2, wb2, xs2, tmp, tmp2, spare, send, recv, load, news):
    nx, ny, nz = sizes
    mx, my, mz = lax.axis_index("gx"), lax.axis_index("gy"), lax.axis_index("gz")
    used = [0]

    def inside(i, j, k):
        tests = []
        if i < 0:
            tests.append(mx + i >= 0)
        if i > 0:
            tests.append(mx + i < nx)
        if j < 0:
            tests.append(my + j >= 0)
        if j > 0:
            tests.append(my + j < ny)
        if k < 0:
            tests.append(mz + k >= 0)
        if k > 0:
            tests.append(mz + k < nz)
        ok = tests[0]
        for test in tests[1:]:
            ok = ok & test
        return ok

    def amount(where, rows, number, sent):
        whole = spare.at[pl.ds(0, rows)]

        @pl.when(where)
        def _():
            copy = pltpu.make_async_remote_copy(
                src_ref=whole, dst_ref=whole, send_sem=send.at[number], recv_sem=recv.at[number],
                device_id=(mx, my, mz), device_id_type=MESH,
            )
            if sent:
                copy.wait_send()
            else:
                copy.wait_recv()

    def waits(number, cases):
        def wait(sent):
            with jax.named_scope(f"{'sent' if sent else 'wait'}{number}"):
                for where, rows in cases:
                    amount(where, rows, number, sent)

        return (lambda: wait(False)), (lambda: wait(True))

    def some(n):
        return (1, 2) if n > 2 else (1,)

    near_x = jnp.where(mx > 0, 1, 0) + jnp.where(mx < nx - 1, 1, 0)
    near_y = jnp.where(my > 0, 1, 0) + jnp.where(my < ny - 1, 1, 0)
    near_z = jnp.where(mz > 0, 1, 0) + jnp.where(mz < nz - 1, 1, 0)
    low_y, high_y = jnp.minimum(my, REACH), jnp.minimum(ny - 1 - my, REACH)
    far_counts = sorted({min(y, REACH) + min(ny - 1 - y, REACH) for y in range(ny)})

    def exchange(moves, face, corner, stack):
        number = used[0]
        used[0] += 1
        for (i, j, k), src, dst in moves:
            copy = pltpu.make_async_remote_copy(
                src_ref=src, dst_ref=dst, send_sem=send.at[number], recv_sem=recv.at[number],
                device_id=(mx + i, my + j, mz + k), device_id_type=MESH,
            )
            pl.when(inside(i, j, k))(copy.start)
        cases = []
        for x in some(nx):
            for y in some(ny):
                for z in some(nz) if stack else (0,):
                    where = (near_x == x) & (near_y == y)
                    if stack:
                        where = where & (near_z == z)
                    cases.append((where, (x + y) * face + x * y * corner + (z * (1 + x) * (stack[0] + y * stack[1]) if stack else 0)))
        return waits(number, cases)

    def far_start(ref, number, shift, j, thin=False):
        first, rows = (W2 + (1 if j > 0 else 0), 1) if thin else (W2, 2)
        planes = pl.ds(P2 + 2 * mx, 2)
        copy = pltpu.make_async_remote_copy(
            src_ref=ref.at[planes, :, pl.ds(first, rows), :], dst_ref=ref.at[planes, :, pl.ds(first - 2 * j, rows), :],
            send_sem=send.at[number], recv_sem=recv.at[number],
            device_id=(lax.rem(mx + shift, nx), my + j, mz), device_id_type=MESH,
        )
        if j == 0:
            copy.start()
        else:
            pl.when(inside(0, j, 0))(copy.start)

    distances = [j for j in sorted(range(-REACH, REACH + 1), key=lambda o: -abs(o)) if abs(j) < ny]

    def column_gather(ref):
        number = used[0]
        used[0] += 1
        for j in distances:
            if j != 0:
                far_start(ref, number, 0, j)
        return waits(number, [(low_y + high_y == c, 4 * c) for c in far_counts])

    def plane_gather(ref):
        number = used[0]
        used[0] += 1
        for j in distances:
            for shift in range(nx):
                if (shift, j) != (0, 0):
                    far_start(ref, number, shift, j, abs(j) == REACH)
        cases = {}
        for y in range(ny):
            c = min(y, REACH) + min(ny - 1 - y, REACH)
            thin = (y >= REACH) + (y + REACH < ny)
            assert cases.setdefault(c, thin) == thin
        return waits(number, [(low_y + high_y == c, 4 * ((1 + c) * nx - 1) - 2 * thin * nx) for c, thin in cases.items()])

    def row_gather(ref):
        number = used[0]
        used[0] += 1
        part = ref.at[pl.ds(P2 + 2 * mx, 2), :, pl.ds(W2 - 2 * REACH, 4 * REACH + 2), :]
        for shift in range(1, nx):
            pltpu.make_async_remote_copy(
                src_ref=part, dst_ref=part, send_sem=send.at[number], recv_sem=recv.at[number],
                device_id=(lax.rem(mx + shift, nx), my, mz), device_id_type=MESH,
            ).start()
        return waits(number, [(mx >= 0, (nx - 1) * 2 * (4 * REACH + 2))])

    def zero(ref):
        ref[...] = jnp.zeros(ref.shape, F32)

    def coarse_of(read, count, rows):
        for tile in range(2):
            for i in range(count):
                total = read(2 * i, 0, tile) + read(2 * i, 1, tile) + read(2 * i + 1, 0, tile) + read(2 * i + 1, 1, tile)
                tmp[tile, rows * i : rows * (i + 1), :] = 0.125 * total
        size = max(8, count * rows)
        lane = lanes_of((size, 128))
        pairs = [tmp[tile, 0:size, :] for tile in range(2)]
        pairs = [p + pltpu.roll(p, 127, 1) for p in pairs]
        index = (2 * lane) % 128
        out = jnp.where(lane < 64, pair_gather(pairs[0], index), pair_gather(pairs[1], index))
        tmp2[0:size, :] = out
        return [tmp2[rows * i : rows * (i + 1), :] for i in range(count)]

    def pack_edges(reads, out):
        for way, (tile, start) in enumerate(((1, 120), (0, 0))):
            packed = jnp.zeros((8, 128), F32)
            lane = lanes_of((8, 128))
            for a, read in enumerate(reads):
                for i in range(8):
                    at = 8 * i + 64 * a
                    part = pltpu.roll(read(i, tile), (at - start) % 128, 1)
                    packed = jnp.where((lane >= at) & (lane < at + 8), part, packed)
            out[way] = packed

    def edge_moves(src, dst, own, width, depth):
        moves = []
        for i, j, k in STACK:
            way, side = (0, 0) if k > 0 else (1, 1)
            rows, there = halo(j, own, width, depth)
            mine_rows = pl.ds(rows.start - own, rows.size)
            moves.append(((i, j, k), src.at[way, mine_rows, :], dst.at[side, 1 - i, there, :]))
        return moves

    def pack_coarse(out):
        lane = lanes_of((4, 128))
        for way, start in enumerate((96, 0)):
            packed = jnp.zeros((4, 128), F32)
            for i in range(4):
                part = pltpu.roll(tmp2[4 * i : 4 * i + 8, :], (32 * i - start) % 128, 1)[0:4]
                packed = jnp.where((lane >= 32 * i) & (lane < 32 * i + 32), part, packed)
            out[way, 0:4] = packed

    def unpack_coarse(src, p):
        lane = lanes_of((24, 128))
        high_end, low_start = jnp.where(mz < nz - 1, 32, 0), jnp.where(mz > 0, 96, 128)
        low = pltpu.roll(src[0, p // 4], (96 - 32 * (p % 4)) % 128, 1)
        high = pltpu.roll(src[1, p // 4], (-32 * (p % 4)) % 128, 1)
        return jnp.where(lane < high_end, high, jnp.where(lane >= low_start, low, 0.0))

    def unpack_edges(src, a, write):
        lane = lanes_of((24, 128))
        high_end, low_start = jnp.where(mz < nz - 1, 8, 0), jnp.where(mz > 0, 120, 128)
        for p in range(2 * P0 + 8):
            group, i = (0, 3 + p) if p < P0 else ((1, p - P0) if p < P0 + 8 else (2, p - P0 - 8))
            at = 8 * i + 64 * a
            low = pltpu.roll(src[0, group], (120 - at) % 128, 1)
            high = pltpu.roll(src[1, group], -at % 128, 1)
            write(p, jnp.where(lane < high_end, high, jnp.where(lane >= low_start, low, 0.0)))

    def halo(step, own, width, depth):
        if step == 0:
            return pl.ds(own, width), pl.ds(own, width)
        if step > 0:
            return pl.ds(own + width - depth, depth), pl.ds(own - depth, depth)
        return pl.ds(own, depth), pl.ds(own + width, depth)

    def fine_moves(ref, depth):
        moves = []
        for i, j, k in DIAGONAL_FIRST:
            (sp, dp), (sr, dr) = halo(i, P0, 8, depth), halo(j, W0, 8, depth)
            moves.append(((i, j, k), ref.at[sp, pl.ds(0, 2), sr, :], ref.at[dp, pl.ds(0, 2), dr, :]))
        return moves

    def coarse_moves(ref, depth, tiles):
        moves = []
        for i, j, k in DIAGONAL_FIRST:
            (sp, dp), (sr, dr) = halo(i, P1, 4, depth), halo(j, W1, 4, depth)
            if tiles:
                moves.append(((i, j, k), ref.at[sp, :, sr, :], ref.at[dp, :, dr, :]))
            else:
                moves.append(((i, j, k), ref.at[sp, sr, :], ref.at[dp, dr, :]))
        return moves

    loads = []
    for a, source in enumerate((b_ref, k_ref)):
        for tile in range(2):
            loads.append(
                pltpu.make_async_copy(
                    source.at[:, :, pl.ds(128 * tile, 128)],
                    ext.at[a, pl.ds(P0, 8), tile, pl.ds(W0, 8), :],
                    load.at[2 * a + tile],
                )
            )
            loads[-1].start()
    barrier = pltpu.get_barrier_semaphore()

    def tell(offsets, semaphore):
        for i, j, k in offsets:

            @pl.when(inside(i, j, k))
            def _():
                pl.semaphore_signal(semaphore, inc=1, device_id=(mx + i, my + j, mz + k), device_id_type=MESH)

    def hear(offsets, semaphore):
        with jax.named_scope("hear"):
            pl.semaphore_wait(semaphore, sum(jnp.where(inside(i, j, k), 1, 0) for i, j, k in offsets))

    for i, j, k in STACK + FLAT:
        ok = inside(i, j, k)
        to = tuple(jnp.where(ok, m + step, m) for m, step in ((mx, i), (my, j), (mz, k)))
        pl.semaphore_signal(barrier, inc=1, device_id=to, device_id_type=MESH)
    zero(tmp)
    zero(tmp2)
    for copy in loads:
        copy.wait()
    pack_edges([lambda i, t: ext[0, P0 + i, t, W0 : W0 + 8, :], lambda i, t: ext[1, P0 + i, t, W0 : W0 + 8, :]], edge_out)
    with jax.named_scope("barrier"):
        pl.semaphore_wait(barrier, 26)
    edges_arrive, edges_left = exchange(edge_moves(edge_out, edge_in, W0, 8, 5), 0, 0, (8, 5))
    moves = []
    for (offset, src_b, dst_b), (_, src_k, dst_k) in zip(fine_moves(ext.at[0], 4), fine_moves(ext.at[1], 5)):
        moves += [(offset, src_b, dst_b), (offset, src_k, dst_k)]
    x0_arrive, x0_left = exchange(moves, 144, 82, None)

    tell(NEXT, news.at[0])

    for ref in (redge_in, rext, bin1, bedge_in, dia1, rex1, xex1):
        zero(ref)
    own_k1 = coarse_of(lambda i, parity, t: ext[1, P0 + i, t, pl.ds(W0 + parity, 4, stride=2), :], 4, 4)
    for i, value in enumerate(own_k1):
        kin1[P1 + i, W1 : W1 + 4, :] = value
    pack_coarse(kedge_out)
    k1_arrive, k1_left = exchange(edge_moves(kedge_out, kedge_in, W1, 4, 4) + coarse_moves(kin1, 4, False), 16, 16, (4, 4))
    for ref in (va0, wa0, vb0, wb0, va1, wa1, vb1, wb1, kap2, va2, wa2, vb2, wb2, xs2):
        zero(ref)
    hear(NEXT, news.at[0])
    tell(OVER, news.at[1])
    hear(OVER, news.at[1])
    tell(FLAT, news.at[2])
    edges_arrive()

    def put(a):
        def write(p, value):
            ext[a, p, 2] = value

        return write

    unpack_edges(edge_in, 0, put(0))
    unpack_edges(edge_in, 1, put(1))
    x0_arrive()
    row = lax.broadcasted_iota(jnp.int32, (24, 128), 0)

    def planes_in(p, own, width):
        return (mx > 0) if p < own else ((mx < nx - 1) if p >= own + width else None)

    def inside_rows(p, own, width, own_row, width_row, depth):
        start = jnp.where(my > 0, own_row - depth, own_row)
        stop = jnp.where(my < ny - 1, own_row + width_row + depth, own_row + width_row)
        ok = planes_in(p, own, width)
        if ok is not None:
            stop = jnp.where(ok, stop, 0)
        return (row >= start) & (row < stop)

    for p in range(18):
        mask = inside_rows(p, P0, 8, W0, 8, 5)
        for tile in range(3):
            kap0[p, tile] = jnp.where(mask, ext[1, p, tile] * (0.5 / 30.0), 0.0)
    theta0, weights0 = chebyshev_coefs(DEGREE, FINE_LOW)
    lo, hi = P0 - 4, P0 + 12

    def start_level(level, planes, row, rows, theta, r_in, r_out, v_ref, w_ref, make_diagonal, size=2):
        kappa, diagonal, inverse = level
        for first, n in chunks(planes[0], planes[1], size):
            at = (pl.ds(first, n), slice(None), pl.ds(row, rows), slice(None))
            kap = kappa[at]
            if make_diagonal:
                dia = 128.0 * kap + stencil_sum(kappa, first, n, row, rows)
                diagonal[at] = dia
            else:
                dia = diagonal[at]
            inv = jnp.where(kap > 0.0, 1.0 / dia, 0.0)
            inverse[at] = inv
            r = jnp.where(kap > 0.0, r_in(at), 0.0)
            r_out[at] = r
            new = (theta * inv) * r
            v_ref[at] = new
            w_ref[at] = kap * new

    level0 = (kap0, dia0, inv0)
    start_level(level0, (lo, hi), 4, 16, theta0, lambda at: ext[(0,) + at], res0, va0, wa0, True, FINE)

    def own0(ref):
        return ref[P0 : P0 + 8, 0:2, W0 : W0 + 8, :]

    xs0[...] = own0(va0)
    here, there = (va0, wa0), (vb0, wb0)

    def smooth0(step, r_in):
        nonlocal here, there
        apply(level0, here, r_in, res0, (P0 - 3 + step, P0 + 11 - step), 4, 16, weights0[step], there, FINE)
        xs0[...] += own0(there[0])
        here, there = there, here

    smooth0(0, lambda at: res0[at])
    smooth0(1, lambda at: res0[at])

    k1_arrive()
    for p in range(12):
        mask = inside_rows(p, P1, 4, W1, 4, 4)
        kap1[p, 0] = jnp.where(mask, kin1[p] * (0.125 / 30.0), 0.0)
        kap1[p, 1] = jnp.where(mask, unpack_coarse(kedge_in, p) * (0.125 / 30.0), 0.0)
    for first, n in chunks(P1, P1 + 4, 2):
        at = (pl.ds(first, n), slice(None), pl.ds(W1, 8), slice(None))
        value = 128.0 * kap1[at] + stencil_sum(kap1, first, n, W1, 8)
        dia1[first : first + n, :, W1 : W1 + 4, :] = value[:, :, 0:4]
    hear(FLAT, news.at[2])
    d1_arrive, d1_left = exchange(coarse_moves(dia1, 4, True), 32, 32, None)
    smooth0(2, lambda at: res0[at])

    def put_rext(first, n, r):
        rext[0, pl.ds(first, n), 0:2, W0 : W0 + 8, :] = r[:, 0:2]

    apply(level0, here, lambda at: res0[at], put_rext, (P0, P0 + 8), W0, 8, None, None, FINE)

    own_b1 = coarse_of(lambda i, parity, t: rext[0, P0 + i, t, pl.ds(W0 + parity, 4, stride=2), :], 4, 4)
    for i, value in enumerate(own_b1):
        bin1[P1 + i, W1 : W1 + 4, :] = value
    pack_coarse(bedge_out)
    b1_arrive, b1_left = exchange(edge_moves(bedge_out, bedge_in, W1, 4, 4) + coarse_moves(bin1, 4, False), 16, 16, (4, 4))
    own_k2 = coarse_of(lambda i, parity, t: kap1[P1 + i, t, pl.ds(W1 + parity, 2, stride=2), :], 2, 2)
    for i, value in enumerate(own_k2):
        kin2[P2 + 2 * mx + i, 0, W2 : W2 + 2, :] = 0.25 * value
    k2_arrive, k2_left = column_gather(kin2)
    pack_edges([lambda i, t: rext[0, P0 + i, t, W0 : W0 + 8, :]], redge_out)
    edges_left()
    x0_left()
    k1_left()
    d1_arrive()
    d1_left()
    b1_arrive()
    for p in range(12):
        res1[p, 0] = bin1[p]
        res1[p, 1] = unpack_coarse(bedge_in, p)
    level1 = (kap1, dia1, inv1)
    start_level(level1, (0, 12), 4, 16, theta0, lambda at: res1[at], res1, va1, wa1, False)

    def own1(ref):
        return ref[P1 : P1 + 4, :, W1 : W1 + 8, :]

    xs1[...] = own1(va1)
    here, there = (va1, wa1), (vb1, wb1)
    for step in range(3):
        at_row, rows = ((4, 16), (6, 8), (7, 8))[step]
        apply(level1, here, lambda at: res1[at], res1, (P1 - 3 + step, P1 + 7 - step), at_row, rows, weights0[step], there)
        xs1[...] += own1(there[0])
        here, there = there, here

    def put_rex1(first, n, r):
        rex1[pl.ds(first, n), :, W1 : W1 + 4, :] = r[:, :, 0:4]

    apply(level1, here, lambda at: res1[at], put_rex1, (P1, P1 + 4), W1, 8, None)

    own_b2 = coarse_of(lambda i, parity, t: rex1[P1 + i, t, pl.ds(W1 + parity, 2, stride=2), :], 2, 2)
    for i, value in enumerate(own_b2):
        bin2[P2 + 2 * mx + i, 0, W2 : W2 + 2, :] = value
    b2_arrive, b2_left = plane_gather(bin2)
    k2_arrive()
    m2_arrive, m2_left = row_gather(kin2)
    r1_arrive, r1_left = exchange(coarse_moves(rex1, 3, True), 24, 18, None)
    r0_arrive, r0_left = exchange(edge_moves(redge_out, redge_in, W0, 8, 4) + fine_moves(rext.at[0], 4), 64, 32, (8, 4))
    k2_left()
    b1_left()
    m2_arrive()
    m2_left()
    full = 2 * nx
    at_row = lax.broadcasted_iota(jnp.int32, (full, 1, 24, 128), 2) + (8 - W2)
    start, stop = jnp.maximum(-2 * REACH, -2 * my), jnp.minimum(2 * REACH + 2, 2 * (ny - my))
    window = (slice(P2, P2 + full), slice(None), slice(8, 32), slice(None))
    kap2[window] = jnp.where((at_row >= start) & (at_row < stop), kin2[window], 0.0)
    theta2, weights2 = chebyshev_coefs(COARSE_DEGREE, COARSE_LOW)
    level2 = (kap2, dia2, inv2)
    b2_arrive()
    start_level(level2, (P2, P2 + full), 8, 24, theta2, lambda at: bin2[at], res2, va2, wa2, True)
    near = (slice(P2, P2 + full), slice(None), slice(W2 - 3, W2 + 5), slice(None))
    xs2[near] = va2[near]
    here, there = (va2, wa2), (vb2, wb2)
    for step in range(COARSE_DEGREE - 1):
        at_row, rows = (8, 24) if step == 0 else ((W2 - 7, 16) if step < 5 else (W2 - 3, 8))
        apply(level2, here, lambda at: res2[at], res2, (P2, P2 + full), at_row, rows, weights2[step], there)
        xs2[near] += there[0][near]
        here, there = there, here

    half = lanes_of((8, 128)) // 2
    for j in range(6):
        coarse = xs2[P2 + 2 * mx - 2 + j, 0, W2 - 2 : W2 + 6, :]
        for tile in range(2):
            value = pair_gather(coarse, half + 64 * tile)[0:6]
            for e in range(2):
                for parity in range(2):
                    va1[2 * j + e, tile, pl.ds(W1 - 4 + parity, 6, stride=2), :] = value
    for first, n in chunks(0, 12, 2):
        wa1[first : first + n] = kap1[first : first + n] * va1[first : first + n]
    xs1[...] += own1(va1)
    r1_arrive()
    here, there = (va1, wa1), (vb1, wb1)
    apply(level1, here, lambda at: rex1[at], res1, (P1 - 3, P1 + 7), 4, 16, (None, theta0), there)
    xs1[...] += own1(there[0])
    here, there = there, here
    for step in range(3):
        at_row = (6, 7, 8)[step]
        apply(level1, here, lambda at: res1[at], res1, (P1 - 2 + step, P1 + 6 - step), at_row, 8, weights0[step], there)
        xs1[...] += own1(there[0])
        here, there = there, here
    xex1[P1 : P1 + 4, :, W1 : W1 + 4, :] = xs1[:, :, 0:4, :]
    x1_arrive, x1_left = exchange(coarse_moves(xex1, 3, True), 24, 18, None)
    b2_left()
    r1_left()
    r0_left()
    r0_arrive()

    def put_rext2(p, value):
        rext[0, p, 2] = value

    unpack_edges(redge_in, 0, put_rext2)
    x1_arrive()
    lane = lanes_of((8, 128))
    ends = jnp.where(lane < 64, half, half + 64)
    for p in range(1, 11):
        for source_row, keep in ((W1 - 4, 8), (W1 + 4, 4)):
            for tile, source_tile, index in ((0, 0, half), (1, 0, half + 64), (2, 1, ends)):
                value = pair_gather(xex1[p, source_tile, source_row : source_row + 8, :], index)[0:keep]
                for q in (2 * p - 3, 2 * p - 2):
                    if 0 <= q < 18:
                        for parity in range(2):
                            va0[q, tile, pl.ds(2 * (source_row - 4) + parity, keep, stride=2), :] = value
    for first, n in chunks(0, 18, 2):
        wa0[first : first + n] = kap0[first : first + n] * va0[first : first + n]
    xs0[...] += own0(va0)
    here, there = (va0, wa0), (vb0, wb0)
    apply(level0, here, lambda at: rext[(0,) + at], res0, (lo, hi), 4, 16, (None, theta0), there, FINE)
    xs0[...] += own0(there[0])
    here, there = there, here
    for step in range(3):
        smooth0(step, lambda at: res0[at])

    def put_out(first, n, r):
        for tile in range(2):
            r_ref[first - P0 : first - P0 + n, :, 128 * tile : 128 * tile + 128] = r[:, tile]

    apply(level0, here, lambda at: res0[at], put_out, (P0, P0 + 8), W0, 8, None, None, FINE)
    for tile in range(2):
        x_ref[:, :, 128 * tile : 128 * tile + 128] = xs0[:, tile]
    x1_left()


def solution(mesh):
    sizes = tuple(mesh.shape[axis] for axis in ("gx", "gy", "gz"))

    def step(conductivity, source):
        def vmem(*shape):
            return pltpu.VMEM(shape, F32)

        level0, level1, level2 = (18, 3, 24, 128), (12, 2, 24, 128), (12, 1, 40, 128)
        sems = 11
        shape = jax.ShapeDtypeStruct(conductivity.shape, F32)
        return pl.pallas_call(
            lambda *refs: kernel(sizes, *refs),
            name="cycle",
            out_shape=(shape, shape),
            in_specs=[pl.BlockSpec(memory_space=pltpu.HBM)] * 2,
            out_specs=(pl.BlockSpec(memory_space=pltpu.VMEM),) * 2,
            scratch_shapes=[
                vmem(2, *level0), vmem(2, 3, 24, 128), vmem(2, 8, 128), vmem(2, 3, 24, 128), vmem(2, 8, 128), vmem(1, *level0),
                *[vmem(*level0) for _ in range(8)], vmem(8, 2, 8, 128),
                vmem(12, 24, 128), vmem(12, 24, 128), *[vmem(*s) for s in 2 * ((2, 3, 24, 128), (2, 8, 128))], *[vmem(*level1) for _ in range(10)], vmem(4, 2, 8, 128),
                *[vmem(*level2) for _ in range(11)],
                vmem(2, 16, 128), vmem(24, 128), vmem(1152, 128),
                pltpu.SemaphoreType.DMA((sems,)), pltpu.SemaphoreType.DMA((sems,)), pltpu.SemaphoreType.DMA((4,)),
                pltpu.SemaphoreType.REGULAR((3,)),
            ],
            compiler_params=pltpu.CompilerParams(
                collective_id=0, has_side_effects=True, vmem_limit_bytes=50 * 1024 * 1024
            ),
        )(*(pltpu.with_memory_space_constraint(v, pltpu.HBM) for v in (conductivity, source)))

    spec = P("gx", "gy", "gz")
    return jax.shard_map(step, mesh=mesh, in_specs=(spec, spec), out_specs=(spec, spec), check_vma=False)
```

```python
import jax
import jax.numpy as jnp
from jax import lax
from jax.experimental import pallas as pl
from jax.experimental.pallas import tpu as pltpu
from jax.sharding import PartitionSpec as P

MESH = pl.DeviceIdType.MESH
F32 = jnp.float32
DEGREE = 4
COARSE_DEGREE = 8
UPPER = 2.0
FINE_LOW = 0.5
COARSE_LOW = 0.03
REACH = 5

P0, W0 = 5, 8
P1, W1 = 4, 8
P2, W2 = 2, 18
SIDES = (-1, 0, 1)
FINE = 7
FLAT = [(i, j, 0) for i in SIDES for j in SIDES if (i, j) != (0, 0)]
STACK = [(i, j, k) for k in (-1, 1) for i in SIDES for j in SIDES]
NEXT, OVER = [(0, -1, 0), (0, 1, 0)], [(0, -2, 0), (0, 2, 0)]
DIAGONAL_FIRST = sorted(FLAT, key=lambda o: -abs(o[0]) - abs(o[1]))


def chebyshev_coefs(degree, lower):
    centre = (UPPER + lower) / 2.0
    half_width = (UPPER - lower) / 2.0
    ratio_term = centre / half_width
    rho_prev = 1.0 / ratio_term
    weights = []
    for _ in range(1, degree):
        rho_next = 1.0 / (2.0 * ratio_term - rho_prev)
        weights.append((rho_next * rho_prev, 2.0 * rho_next / half_width))
        rho_prev = rho_next
    return 1.0 / centre, weights


def rolled(values, shift):
    flat = values.reshape(-1, 128)
    return pltpu.roll(flat, shift % 128, 1).reshape(values.shape)


def lanes_of(shape):
    return lax.broadcasted_iota(jnp.int32, shape, len(shape) - 1)


def beside(values):
    up, down = rolled(values, 1), rolled(values, -1)
    tiles = values.shape[1]
    if tiles > 1:
        lane = lanes_of(values.shape)
        before = jnp.concatenate([up[:, tiles - 1 :], up[:, : tiles - 1]], axis=1)
        after = jnp.concatenate([down[:, 1:], down[:, :1]], axis=1)
        up = jnp.where(lane == 0, before, up)
        down = jnp.where(lane == 127, after, down)
    return up + down


def stencil_sum(ref, first, count, row, rows):
    planes = pl.ds(first - 1, count + 2)
    centre = ref[planes, :, pl.ds(row, rows), :]
    side = ref[planes, :, pl.ds(row - 1, rows), :] + ref[planes, :, pl.ds(row + 1, rows), :]
    corner = 3.0 * centre + side
    face = 14.0 * centre + 3.0 * side
    outer = face[1:-1] + corner[:-2] + corner[2:]
    middle = 14.0 * side[1:-1] + face[:-2] + face[2:]
    return middle + beside(outer)


def chunks(first, last, size):
    return [(at, min(size, last - at)) for at in range(first, last, size)]


def apply(level, source, r_in, r_out, planes, row, rows, coefs, target=None, size=2):
    kappa, diagonal, inverse = level
    v_ref, w_ref = source
    for first, count in chunks(planes[0], planes[1], size):
        at = (pl.ds(first, count), slice(None), pl.ds(row, rows), slice(None))
        v = v_ref[at]
        r = r_in(at) - diagonal[at] * v
        r = r + kappa[at] * stencil_sum(v_ref, first, count, row, rows)
        r = r + stencil_sum(w_ref, first, count, row, rows)
        if callable(r_out):
            r_out(first, count, r)
        else:
            r_out[at] = r
        if coefs is not None:
            new = (coefs[1] * inverse[at]) * r
            if coefs[0] is not None:
                new = new + coefs[0] * v
            target[0][at] = new
            target[1][at] = kappa[at] * new


def pair_gather(values, index):
    return jnp.take_along_axis(values, index, axis=1)


def kernel(sizes, k_ref, b_ref, x_ref, r_ref, ext, edge_in, edge_out, redge_in, redge_out, rext,
           kap0, dia0, inv0, res0, va0, wa0, vb0, wb0, xs0,
           kin1, bin1, kedge_in, kedge_out, bedge_in, bedge_out, kap1, dia1, inv1, res1, va1, wa1, vb1, wb1, rex1, xex1, xs1,
           kin2, kap2, dia2, inv2, bin2, res2, va2, wa2, vb2, wb2, xs2, tmp, tmp2, spare, send, recv, load, news):
    nx, ny, nz = sizes
    mx, my, mz = lax.axis_index("gx"), lax.axis_index("gy"), lax.axis_index("gz")
    used = [0]

    def inside(i, j, k):
        tests = []
        if i < 0:
            tests.append(mx + i >= 0)
        if i > 0:
            tests.append(mx + i < nx)
        if j < 0:
            tests.append(my + j >= 0)
        if j > 0:
            tests.append(my + j < ny)
        if k < 0:
            tests.append(mz + k >= 0)
        if k > 0:
            tests.append(mz + k < nz)
        ok = tests[0]
        for test in tests[1:]:
            ok = ok & test
        return ok

    def amount(where, rows, number, sent):
        whole = spare.at[pl.ds(0, rows)]

        @pl.when(where)
        def _():
            copy = pltpu.make_async_remote_copy(
                src_ref=whole, dst_ref=whole, send_sem=send.at[number], recv_sem=recv.at[number],
                device_id=(mx, my, mz), device_id_type=MESH,
            )
            if sent:
                copy.wait_send()
            else:
                copy.wait_recv()

    def waits(number, cases):
        def wait(sent):
            with jax.named_scope(f"{'sent' if sent else 'wait'}{number}"):
                for where, rows in cases:
                    amount(where, rows, number, sent)

        return (lambda: wait(False)), (lambda: wait(True))

    def some(n):
        return (1, 2) if n > 2 else (1,)

    near_x = jnp.where(mx > 0, 1, 0) + jnp.where(mx < nx - 1, 1, 0)
    near_y = jnp.where(my > 0, 1, 0) + jnp.where(my < ny - 1, 1, 0)
    near_z = jnp.where(mz > 0, 1, 0) + jnp.where(mz < nz - 1, 1, 0)
    low_y, high_y = jnp.minimum(my, REACH), jnp.minimum(ny - 1 - my, REACH)
    far_counts = sorted({min(y, REACH) + min(ny - 1 - y, REACH) for y in range(ny)})

    def exchange(moves, face, corner, stack):
        number = used[0]
        used[0] += 1
        for (i, j, k), src, dst in moves:
            copy = pltpu.make_async_remote_copy(
                src_ref=src, dst_ref=dst, send_sem=send.at[number], recv_sem=recv.at[number],
                device_id=(mx + i, my + j, mz + k), device_id_type=MESH,
            )
            pl.when(inside(i, j, k))(copy.start)
        cases = []
        for x in some(nx):
            for y in some(ny):
                for z in some(nz) if stack else (0,):
                    where = (near_x == x) & (near_y == y)
                    if stack:
                        where = where & (near_z == z)
                    cases.append((where, (x + y) * face + x * y * corner + (z * (1 + x) * (stack[0] + y * stack[1]) if stack else 0)))
        return waits(number, cases)

    def far_start(ref, number, shift, j, thin=False):
        first, rows = (W2 + (1 if j > 0 else 0), 1) if thin else (W2, 2)
        planes = pl.ds(P2 + 2 * mx, 2)
        copy = pltpu.make_async_remote_copy(
            src_ref=ref.at[planes, :, pl.ds(first, rows), :], dst_ref=ref.at[planes, :, pl.ds(first - 2 * j, rows), :],
            send_sem=send.at[number], recv_sem=recv.at[number],
            device_id=(lax.rem(mx + shift, nx), my + j, mz), device_id_type=MESH,
        )
        if j == 0:
            copy.start()
        else:
            pl.when(inside(0, j, 0))(copy.start)

    distances = [j for j in sorted(range(-REACH, REACH + 1), key=lambda o: -abs(o)) if abs(j) < ny]

    def column_gather(ref):
        number = used[0]
        used[0] += 1
        for j in distances:
            if j != 0:
                far_start(ref, number, 0, j)
        return waits(number, [(low_y + high_y == c, 4 * c) for c in far_counts])

    def plane_gather(ref):
        number = used[0]
        used[0] += 1
        for j in distances:
            for shift in range(nx):
                if (shift, j) != (0, 0):
                    far_start(ref, number, shift, j, abs(j) == REACH)
        thin_y = jnp.where(my >= REACH, 1, 0) + jnp.where(my + REACH < ny, 1, 0)
        cases = sorted({(min(y, REACH) + min(ny - 1 - y, REACH), (y >= REACH) + (y + REACH < ny)) for y in range(ny)})
        return waits(
            number,
            [((low_y + high_y == c) & (thin_y == t), 4 * ((1 + c) * nx - 1) - 2 * t * nx) for c, t in cases],
        )

    def row_gather(ref):
        number = used[0]
        used[0] += 1
        part = ref.at[pl.ds(P2 + 2 * mx, 2), :, pl.ds(W2 - 2 * REACH, 4 * REACH + 2), :]
        for shift in range(1, nx):
            pltpu.make_async_remote_copy(
                src_ref=part, dst_ref=part, send_sem=send.at[number], recv_sem=recv.at[number],
                device_id=(lax.rem(mx + shift, nx), my, mz), device_id_type=MESH,
            ).start()
        return waits(number, [(mx >= 0, (nx - 1) * 2 * (4 * REACH + 2))])

    def zero(ref):
        ref[...] = jnp.zeros(ref.shape, F32)

    def coarse_of(read, count, rows):
        for tile in range(2):
            for i in range(count):
                total = read(2 * i, 0, tile) + read(2 * i, 1, tile) + read(2 * i + 1, 0, tile) + read(2 * i + 1, 1, tile)
                tmp[tile, rows * i : rows * (i + 1), :] = 0.125 * total
        size = max(8, count * rows)
        lane = lanes_of((size, 128))
        pairs = [tmp[tile, 0:size, :] for tile in range(2)]
        pairs = [p + pltpu.roll(p, 127, 1) for p in pairs]
        index = (2 * lane) % 128
        out = jnp.where(lane < 64, pair_gather(pairs[0], index), pair_gather(pairs[1], index))
        tmp2[0:size, :] = out
        return [tmp2[rows * i : rows * (i + 1), :] for i in range(count)]

    def pack_edges(reads, out):
        for way, (tile, start) in enumerate(((1, 120), (0, 0))):
            packed = jnp.zeros((8, 128), F32)
            lane = lanes_of((8, 128))
            for a, read in enumerate(reads):
                for i in range(8):
                    at = 8 * i + 64 * a
                    part = pltpu.roll(read(i, tile), (at - start) % 128, 1)
                    packed = jnp.where((lane >= at) & (lane < at + 8), part, packed)
            out[way] = packed

    def edge_moves(src, dst, own, width, depth):
        moves = []
        for i, j, k in STACK:
            way, side = (0, 0) if k > 0 else (1, 1)
            rows, there = halo(j, own, width, depth)
            mine_rows = pl.ds(rows.start - own, rows.size)
            moves.append(((i, j, k), src.at[way, mine_rows, :], dst.at[side, 1 - i, there, :]))
        return moves

    def pack_coarse(out):
        lane = lanes_of((4, 128))
        for way, start in enumerate((96, 0)):
            packed = jnp.zeros((4, 128), F32)
            for i in range(4):
                part = pltpu.roll(tmp2[4 * i : 4 * i + 8, :], (32 * i - start) % 128, 1)[0:4]
                packed = jnp.where((lane >= 32 * i) & (lane < 32 * i + 32), part, packed)
            out[way, 0:4] = packed

    def unpack_coarse(src, p):
        lane = lanes_of((24, 128))
        high_end, low_start = jnp.where(mz < nz - 1, 32, 0), jnp.where(mz > 0, 96, 128)
        low = pltpu.roll(src[0, p // 4], (96 - 32 * (p % 4)) % 128, 1)
        high = pltpu.roll(src[1, p // 4], (-32 * (p % 4)) % 128, 1)
        return jnp.where(lane < high_end, high, jnp.where(lane >= low_start, low, 0.0))

    def unpack_edges(src, a, write):
        lane = lanes_of((24, 128))
        high_end, low_start = jnp.where(mz < nz - 1, 8, 0), jnp.where(mz > 0, 120, 128)
        for p in range(2 * P0 + 8):
            group, i = (0, 3 + p) if p < P0 else ((1, p - P0) if p < P0 + 8 else (2, p - P0 - 8))
            at = 8 * i + 64 * a
            low = pltpu.roll(src[0, group], (120 - at) % 128, 1)
            high = pltpu.roll(src[1, group], -at % 128, 1)
            write(p, jnp.where(lane < high_end, high, jnp.where(lane >= low_start, low, 0.0)))

    def halo(step, own, width, depth):
        if step == 0:
            return pl.ds(own, width), pl.ds(own, width)
        if step > 0:
            return pl.ds(own + width - depth, depth), pl.ds(own - depth, depth)
        return pl.ds(own, depth), pl.ds(own + width, depth)

    def fine_moves(ref, depth):
        moves = []
        for i, j, k in DIAGONAL_FIRST:
            (sp, dp), (sr, dr) = halo(i, P0, 8, depth), halo(j, W0, 8, depth)
            moves.append(((i, j, k), ref.at[sp, pl.ds(0, 2), sr, :], ref.at[dp, pl.ds(0, 2), dr, :]))
        return moves

    def coarse_moves(ref, depth, tiles):
        moves = []
        for i, j, k in DIAGONAL_FIRST:
            (sp, dp), (sr, dr) = halo(i, P1, 4, depth), halo(j, W1, 4, depth)
            if tiles:
                moves.append(((i, j, k), ref.at[sp, :, sr, :], ref.at[dp, :, dr, :]))
            else:
                moves.append(((i, j, k), ref.at[sp, sr, :], ref.at[dp, dr, :]))
        return moves

    loads = []
    for a, source in enumerate((b_ref, k_ref)):
        for tile in range(2):
            loads.append(
                pltpu.make_async_copy(
                    source.at[:, :, pl.ds(128 * tile, 128)],
                    ext.at[a, pl.ds(P0, 8), tile, pl.ds(W0, 8), :],
                    load.at[2 * a + tile],
                )
            )
            loads[-1].start()
    barrier = pltpu.get_barrier_semaphore()

    def tell(offsets, semaphore):
        for i, j, k in offsets:

            @pl.when(inside(i, j, k))
            def _():
                pl.semaphore_signal(semaphore, inc=1, device_id=(mx + i, my + j, mz + k), device_id_type=MESH)

    def hear(offsets, semaphore):
        with jax.named_scope("hear"):
            pl.semaphore_wait(semaphore, sum(jnp.where(inside(i, j, k), 1, 0) for i, j, k in offsets))

    for i, j, k in STACK + FLAT:
        ok = inside(i, j, k)
        to = tuple(jnp.where(ok, m + step, m) for m, step in ((mx, i), (my, j), (mz, k)))
        pl.semaphore_signal(barrier, inc=1, device_id=to, device_id_type=MESH)
    zero(tmp)
    zero(tmp2)
    for copy in loads:
        copy.wait()
    pack_edges([lambda i, t: ext[0, P0 + i, t, W0 : W0 + 8, :], lambda i, t: ext[1, P0 + i, t, W0 : W0 + 8, :]], edge_out)
    with jax.named_scope("barrier"):
        pl.semaphore_wait(barrier, 26)
    edges_arrive, edges_left = exchange(edge_moves(edge_out, edge_in, W0, 8, 5), 0, 0, (8, 5))
    moves = []
    for (offset, src_b, dst_b), (_, src_k, dst_k) in zip(fine_moves(ext.at[0], 4), fine_moves(ext.at[1], 5)):
        moves += [(offset, src_b, dst_b), (offset, src_k, dst_k)]
    x0_arrive, x0_left = exchange(moves, 144, 82, None)

    tell(NEXT, news.at[0])

    for ref in (redge_in, rext, bin1, bedge_in, dia1, rex1, xex1):
        zero(ref)
    own_k1 = coarse_of(lambda i, parity, t: ext[1, P0 + i, t, pl.ds(W0 + parity, 4, stride=2), :], 4, 4)
    for i, value in enumerate(own_k1):
        kin1[P1 + i, W1 : W1 + 4, :] = value
    pack_coarse(kedge_out)
    k1_arrive, k1_left = exchange(edge_moves(kedge_out, kedge_in, W1, 4, 4) + coarse_moves(kin1, 4, False), 16, 16, (4, 4))
    for ref in (va0, wa0, vb0, wb0, va1, wa1, vb1, wb1, kap2, va2, wa2, vb2, wb2, xs2):
        zero(ref)
    hear(NEXT, news.at[0])
    tell(OVER, news.at[1])
    hear(OVER, news.at[1])
    tell(FLAT, news.at[2])
    edges_arrive()

    def put(a):
        def write(p, value):
            ext[a, p, 2] = value

        return write

    unpack_edges(edge_in, 0, put(0))
    unpack_edges(edge_in, 1, put(1))
    x0_arrive()
    row = lax.broadcasted_iota(jnp.int32, (24, 128), 0)

    def planes_in(p, own, width):
        return (mx > 0) if p < own else ((mx < nx - 1) if p >= own + width else None)

    def inside_rows(p, own, width, own_row, width_row, depth):
        start = jnp.where(my > 0, own_row - depth, own_row)
        stop = jnp.where(my < ny - 1, own_row + width_row + depth, own_row + width_row)
        ok = planes_in(p, own, width)
        if ok is not None:
            stop = jnp.where(ok, stop, 0)
        return (row >= start) & (row < stop)

    for p in range(18):
        mask = inside_rows(p, P0, 8, W0, 8, 5)
        for tile in range(3):
            kap0[p, tile] = jnp.where(mask, ext[1, p, tile] * (0.5 / 30.0), 0.0)
    theta0, weights0 = chebyshev_coefs(DEGREE, FINE_LOW)
    lo, hi = P0 - 4, P0 + 12

    def start_level(level, planes, row, rows, theta, r_in, r_out, v_ref, w_ref, make_diagonal, size=2):
        kappa, diagonal, inverse = level
        for first, n in chunks(planes[0], planes[1], size):
            at = (pl.ds(first, n), slice(None), pl.ds(row, rows), slice(None))
            kap = kappa[at]
            if make_diagonal:
                dia = 128.0 * kap + stencil_sum(kappa, first, n, row, rows)
                diagonal[at] = dia
            else:
                dia = diagonal[at]
            inv = jnp.where(kap > 0.0, 1.0 / dia, 0.0)
            inverse[at] = inv
            r = jnp.where(kap > 0.0, r_in(at), 0.0)
            r_out[at] = r
            new = (theta * inv) * r
            v_ref[at] = new
            w_ref[at] = kap * new

    level0 = (kap0, dia0, inv0)
    start_level(level0, (lo, hi), 4, 16, theta0, lambda at: ext[(0,) + at], res0, va0, wa0, True, FINE)

    def own0(ref):
        return ref[P0 : P0 + 8, 0:2, W0 : W0 + 8, :]

    xs0[...] = own0(va0)
    here, there = (va0, wa0), (vb0, wb0)

    def smooth0(step, r_in):
        nonlocal here, there
        apply(level0, here, r_in, res0, (P0 - 3 + step, P0 + 11 - step), 4, 16, weights0[step], there, FINE)
        xs0[...] += own0(there[0])
        here, there = there, here

    smooth0(0, lambda at: res0[at])
    smooth0(1, lambda at: res0[at])

    k1_arrive()
    for p in range(12):
        mask = inside_rows(p, P1, 4, W1, 4, 4)
        kap1[p, 0] = jnp.where(mask, kin1[p] * (0.125 / 30.0), 0.0)
        kap1[p, 1] = jnp.where(mask, unpack_coarse(kedge_in, p) * (0.125 / 30.0), 0.0)
    for first, n in chunks(P1, P1 + 4, 2):
        at = (pl.ds(first, n), slice(None), pl.ds(W1, 8), slice(None))
        value = 128.0 * kap1[at] + stencil_sum(kap1, first, n, W1, 8)
        dia1[first : first + n, :, W1 : W1 + 4, :] = value[:, :, 0:4]
    hear(FLAT, news.at[2])
    d1_arrive, d1_left = exchange(coarse_moves(dia1, 4, True), 32, 32, None)
    smooth0(2, lambda at: res0[at])

    def put_rext(first, n, r):
        rext[0, pl.ds(first, n), 0:2, W0 : W0 + 8, :] = r[:, 0:2]

    apply(level0, here, lambda at: res0[at], put_rext, (P0, P0 + 8), W0, 8, None, None, FINE)

    own_b1 = coarse_of(lambda i, parity, t: rext[0, P0 + i, t, pl.ds(W0 + parity, 4, stride=2), :], 4, 4)
    for i, value in enumerate(own_b1):
        bin1[P1 + i, W1 : W1 + 4, :] = value
    pack_coarse(bedge_out)
    b1_arrive, b1_left = exchange(edge_moves(bedge_out, bedge_in, W1, 4, 4) + coarse_moves(bin1, 4, False), 16, 16, (4, 4))
    own_k2 = coarse_of(lambda i, parity, t: kap1[P1 + i, t, pl.ds(W1 + parity, 2, stride=2), :], 2, 2)
    for i, value in enumerate(own_k2):
        kin2[P2 + 2 * mx + i, 0, W2 : W2 + 2, :] = 0.25 * value
    k2_arrive, k2_left = column_gather(kin2)
    pack_edges([lambda i, t: rext[0, P0 + i, t, W0 : W0 + 8, :]], redge_out)
    edges_left()
    x0_left()
    k1_left()
    d1_arrive()
    d1_left()
    b1_arrive()
    for p in range(12):
        res1[p, 0] = bin1[p]
        res1[p, 1] = unpack_coarse(bedge_in, p)
    level1 = (kap1, dia1, inv1)
    start_level(level1, (0, 12), 4, 16, theta0, lambda at: res1[at], res1, va1, wa1, False)

    def own1(ref):
        return ref[P1 : P1 + 4, :, W1 : W1 + 8, :]

    xs1[...] = own1(va1)
    here, there = (va1, wa1), (vb1, wb1)
    for step in range(3):
        at_row, rows = ((4, 16), (6, 8), (7, 8))[step]
        apply(level1, here, lambda at: res1[at], res1, (P1 - 3 + step, P1 + 7 - step), at_row, rows, weights0[step], there)
        xs1[...] += own1(there[0])
        here, there = there, here

    def put_rex1(first, n, r):
        rex1[pl.ds(first, n), :, W1 : W1 + 4, :] = r[:, :, 0:4]

    apply(level1, here, lambda at: res1[at], put_rex1, (P1, P1 + 4), W1, 8, None)

    own_b2 = coarse_of(lambda i, parity, t: rex1[P1 + i, t, pl.ds(W1 + parity, 2, stride=2), :], 2, 2)
    for i, value in enumerate(own_b2):
        bin2[P2 + 2 * mx + i, 0, W2 : W2 + 2, :] = value
    b2_arrive, b2_left = plane_gather(bin2)
    k2_arrive()
    m2_arrive, m2_left = row_gather(kin2)
    r1_arrive, r1_left = exchange(coarse_moves(rex1, 3, True), 24, 18, None)
    r0_arrive, r0_left = exchange(edge_moves(redge_out, redge_in, W0, 8, 4) + fine_moves(rext.at[0], 4), 64, 32, (8, 4))
    k2_left()
    b1_left()
    m2_arrive()
    m2_left()
    full = 2 * nx
    at_row = lax.broadcasted_iota(jnp.int32, (full, 1, 24, 128), 2) + (8 - W2)
    start, stop = jnp.maximum(-2 * REACH, -2 * my), jnp.minimum(2 * REACH + 2, 2 * (ny - my))
    window = (slice(P2, P2 + full), slice(None), slice(8, 32), slice(None))
    kap2[window] = jnp.where((at_row >= start) & (at_row < stop), kin2[window], 0.0)
    theta2, weights2 = chebyshev_coefs(COARSE_DEGREE, COARSE_LOW)
    level2 = (kap2, dia2, inv2)
    b2_arrive()
    start_level(level2, (P2, P2 + full), 8, 24, theta2, lambda at: bin2[at], res2, va2, wa2, True)
    near = (slice(P2, P2 + full), slice(None), slice(W2 - 3, W2 + 5), slice(None))
    xs2[near] = va2[near]
    here, there = (va2, wa2), (vb2, wb2)
    for step in range(COARSE_DEGREE - 1):
        at_row, rows = (8, 24) if step == 0 else ((W2 - 7, 16) if step < 5 else (W2 - 3, 8))
        apply(level2, here, lambda at: res2[at], res2, (P2, P2 + full), at_row, rows, weights2[step], there)
        xs2[near] += there[0][near]
        here, there = there, here

    half = lanes_of((8, 128)) // 2
    for j in range(6):
        coarse = xs2[P2 + 2 * mx - 2 + j, 0, W2 - 2 : W2 + 6, :]
        for tile in range(2):
            value = pair_gather(coarse, half + 64 * tile)[0:6]
            for e in range(2):
                for parity in range(2):
                    va1[2 * j + e, tile, pl.ds(W1 - 4 + parity, 6, stride=2), :] = value
    for first, n in chunks(0, 12, 2):
        wa1[first : first + n] = kap1[first : first + n] * va1[first : first + n]
    xs1[...] += own1(va1)
    r1_arrive()
    here, there = (va1, wa1), (vb1, wb1)
    apply(level1, here, lambda at: rex1[at], res1, (P1 - 3, P1 + 7), 4, 16, (None, theta0), there)
    xs1[...] += own1(there[0])
    here, there = there, here
    for step in range(3):
        at_row = (6, 7, 8)[step]
        apply(level1, here, lambda at: res1[at], res1, (P1 - 2 + step, P1 + 6 - step), at_row, 8, weights0[step], there)
        xs1[...] += own1(there[0])
        here, there = there, here
    xex1[P1 : P1 + 4, :, W1 : W1 + 4, :] = xs1[:, :, 0:4, :]
    x1_arrive, x1_left = exchange(coarse_moves(xex1, 3, True), 24, 18, None)
    b2_left()
    r1_left()
    r0_left()
    r0_arrive()

    def put_rext2(p, value):
        rext[0, p, 2] = value

    unpack_edges(redge_in, 0, put_rext2)
    x1_arrive()
    lane = lanes_of((8, 128))
    ends = jnp.where(lane < 64, half, half + 64)
    for p in range(1, 11):
        for source_row, keep in ((W1 - 4, 8), (W1 + 4, 4)):
            for tile, source_tile, index in ((0, 0, half), (1, 0, half + 64), (2, 1, ends)):
                value = pair_gather(xex1[p, source_tile, source_row : source_row + 8, :], index)[0:keep]
                for q in (2 * p - 3, 2 * p - 2):
                    if 0 <= q < 18:
                        for parity in range(2):
                            va0[q, tile, pl.ds(2 * (source_row - 4) + parity, keep, stride=2), :] = value
    for first, n in chunks(0, 18, 2):
        wa0[first : first + n] = kap0[first : first + n] * va0[first : first + n]
    xs0[...] += own0(va0)
    here, there = (va0, wa0), (vb0, wb0)
    apply(level0, here, lambda at: rext[(0,) + at], res0, (lo, hi), 4, 16, (None, theta0), there, FINE)
    xs0[...] += own0(there[0])
    here, there = there, here
    for step in range(3):
        smooth0(step, lambda at: res0[at])

    def put_out(first, n, r):
        for tile in range(2):
            r_ref[first - P0 : first - P0 + n, :, 128 * tile : 128 * tile + 128] = r[:, tile]

    apply(level0, here, lambda at: res0[at], put_out, (P0, P0 + 8), W0, 8, None, None, FINE)
    for tile in range(2):
        x_ref[:, :, 128 * tile : 128 * tile + 128] = xs0[:, tile]
    x1_left()


def solution(mesh):
    sizes = tuple(mesh.shape[axis] for axis in ("gx", "gy", "gz"))

    def step(conductivity, source):
        def vmem(*shape):
            return pltpu.VMEM(shape, F32)

        level0, level1, level2 = (18, 3, 24, 128), (12, 2, 24, 128), (12, 1, 40, 128)
        sems = 11
        shape = jax.ShapeDtypeStruct(conductivity.shape, F32)
        return pl.pallas_call(
            lambda *refs: kernel(sizes, *refs),
            name="cycle",
            out_shape=(shape, shape),
            in_specs=[pl.BlockSpec(memory_space=pltpu.HBM)] * 2,
            out_specs=(pl.BlockSpec(memory_space=pltpu.VMEM),) * 2,
            scratch_shapes=[
                vmem(2, *level0), vmem(2, 3, 24, 128), vmem(2, 8, 128), vmem(2, 3, 24, 128), vmem(2, 8, 128), vmem(1, *level0),
                *[vmem(*level0) for _ in range(4)], vmem(19, 3, 24, 128), *[vmem(*level0) for _ in range(3)], vmem(8, 2, 8, 128),
                vmem(12, 24, 128), vmem(12, 24, 128), *[vmem(*s) for s in 2 * ((2, 3, 24, 128), (2, 8, 128))], *[vmem(*level1) for _ in range(10)], vmem(4, 2, 8, 128),
                *[vmem(*level2) for _ in range(11)],
                vmem(2, 24, 128), vmem(24, 128), vmem(1152, 128),
                pltpu.SemaphoreType.DMA((sems,)), pltpu.SemaphoreType.DMA((sems,)), pltpu.SemaphoreType.DMA((4,)),
                pltpu.SemaphoreType.REGULAR((3,)),
            ],
            compiler_params=pltpu.CompilerParams(
                collective_id=0, has_side_effects=True, vmem_limit_bytes=50 * 1024 * 1024
            ),
        )(*(pltpu.with_memory_space_constraint(v, pltpu.HBM) for v in (conductivity, source)))

    spec = P("gx", "gy", "gz")
    return jax.shard_map(step, mesh=mesh, in_specs=(spec, spec), out_specs=(spec, spec), check_vma=False)
```

```python
import jax
import jax.numpy as jnp
from jax import lax
from jax.experimental import pallas as pl
from jax.experimental.pallas import tpu as pltpu
from jax.sharding import PartitionSpec as P

MESH = pl.DeviceIdType.MESH
F32 = jnp.float32
DEGREE = 4
COARSE_DEGREE = 8
UPPER = 2.0
FINE_LOW = 0.5
COARSE_LOW = 0.03
REACH = 5

P0, W0 = 5, 8
P1, W1 = 4, 8
P2, W2 = 2, 18
SIDES = (-1, 0, 1)
FINE = 7
FLAT = [(i, j, 0) for i in SIDES for j in SIDES if (i, j) != (0, 0)]
STACK = [(i, j, k) for k in (-1, 1) for i in SIDES for j in SIDES]
NEXT, OVER = [(0, -1, 0), (0, 1, 0)], [(0, -2, 0), (0, 2, 0)]
DIAGONAL_FIRST = sorted(FLAT, key=lambda o: -abs(o[0]) - abs(o[1]))


def chebyshev_coefs(degree, lower):
    centre = (UPPER + lower) / 2.0
    half_width = (UPPER - lower) / 2.0
    ratio_term = centre / half_width
    rho_prev = 1.0 / ratio_term
    weights = []
    for _ in range(1, degree):
        rho_next = 1.0 / (2.0 * ratio_term - rho_prev)
        weights.append((rho_next * rho_prev, 2.0 * rho_next / half_width))
        rho_prev = rho_next
    return 1.0 / centre, weights


def rolled(values, shift):
    flat = values.reshape(-1, 128)
    return pltpu.roll(flat, shift % 128, 1).reshape(values.shape)


def lanes_of(shape):
    return lax.broadcasted_iota(jnp.int32, shape, len(shape) - 1)


def beside(values):
    up, down = rolled(values, 1), rolled(values, -1)
    tiles = values.shape[1]
    if tiles > 1:
        lane = lanes_of(values.shape)
        before = jnp.concatenate([up[:, tiles - 1 :], up[:, : tiles - 1]], axis=1)
        after = jnp.concatenate([down[:, 1:], down[:, :1]], axis=1)
        up = jnp.where(lane == 0, before, up)
        down = jnp.where(lane == 127, after, down)
    return up + down


def stencil_sum(ref, first, count, row, rows):
    planes = pl.ds(first - 1, count + 2)
    centre = ref[planes, :, pl.ds(row, rows), :]
    side = ref[planes, :, pl.ds(row - 1, rows), :] + ref[planes, :, pl.ds(row + 1, rows), :]
    corner = 3.0 * centre + side
    face = 14.0 * centre + 3.0 * side
    outer = face[1:-1] + corner[:-2] + corner[2:]
    middle = 14.0 * side[1:-1] + face[:-2] + face[2:]
    return middle + beside(outer)


def chunks(first, last, size):
    return [(at, min(size, last - at)) for at in range(first, last, size)]


def apply(level, source, r_in, r_out, planes, row, rows, coefs, target=None, size=3):
    kappa, diagonal, inverse = level
    v_ref, w_ref = source
    for first, count in chunks(planes[0], planes[1], size):
        at = (pl.ds(first, count), slice(None), pl.ds(row, rows), slice(None))
        v = v_ref[at]
        r = r_in(at) - diagonal[at] * v
        r = r + kappa[at] * stencil_sum(v_ref, first, count, row, rows)
        r = r + stencil_sum(w_ref, first, count, row, rows)
        if callable(r_out):
            r_out(first, count, r)
        else:
            r_out[at] = r
        if coefs is not None:
            new = (coefs[1] * inverse[at]) * r
            if coefs[0] is not None:
                new = new + coefs[0] * v
            target[0][at] = new
            target[1][at] = kappa[at] * new


def pair_gather(values, index):
    return jnp.take_along_axis(values, index, axis=1)


def kernel(sizes, k_ref, b_ref, x_ref, r_ref, ext, edge_in, edge_out, redge_in, redge_out, rext,
           kap0, dia0, inv0, res0, va0, wa0, vb0, wb0, xs0,
           kin1, bin1, kedge_in, kedge_out, bedge_in, bedge_out, kap1, dia1, inv1, res1, va1, wa1, vb1, wb1, rex1, xex1, xs1,
           kin2, kap2, dia2, inv2, bin2, res2, va2, wa2, vb2, wb2, xs2, tmp, tmp2, spare, send, recv, load, news):
    nx, ny, nz = sizes
    mx, my, mz = lax.axis_index("gx"), lax.axis_index("gy"), lax.axis_index("gz")
    used = [0]

    def inside(i, j, k):
        tests = []
        if i < 0:
            tests.append(mx + i >= 0)
        if i > 0:
            tests.append(mx + i < nx)
        if j < 0:
            tests.append(my + j >= 0)
        if j > 0:
            tests.append(my + j < ny)
        if k < 0:
            tests.append(mz + k >= 0)
        if k > 0:
            tests.append(mz + k < nz)
        ok = tests[0]
        for test in tests[1:]:
            ok = ok & test
        return ok

    def amount(where, rows, number, sent):
        whole = spare.at[pl.ds(0, rows)]

        @pl.when(where)
        def _():
            copy = pltpu.make_async_remote_copy(
                src_ref=whole, dst_ref=whole, send_sem=send.at[number], recv_sem=recv.at[number],
                device_id=(mx, my, mz), device_id_type=MESH,
            )
            if sent:
                copy.wait_send()
            else:
                copy.wait_recv()

    def waits(number, cases):
        def wait(sent):
            with jax.named_scope(f"{'sent' if sent else 'wait'}{number}"):
                for where, rows in cases:
                    amount(where, rows, number, sent)

        return (lambda: wait(False)), (lambda: wait(True))

    def some(n):
        return (1, 2) if n > 2 else (1,)

    near_x = jnp.where(mx > 0, 1, 0) + jnp.where(mx < nx - 1, 1, 0)
    near_y = jnp.where(my > 0, 1, 0) + jnp.where(my < ny - 1, 1, 0)
    near_z = jnp.where(mz > 0, 1, 0) + jnp.where(mz < nz - 1, 1, 0)
    low_y, high_y = jnp.minimum(my, REACH), jnp.minimum(ny - 1 - my, REACH)
    far_counts = sorted({min(y, REACH) + min(ny - 1 - y, REACH) for y in range(ny)})

    def exchange(moves, face, corner, stack):
        number = used[0]
        used[0] += 1
        for (i, j, k), src, dst in moves:
            copy = pltpu.make_async_remote_copy(
                src_ref=src, dst_ref=dst, send_sem=send.at[number], recv_sem=recv.at[number],
                device_id=(mx + i, my + j, mz + k), device_id_type=MESH,
            )
            pl.when(inside(i, j, k))(copy.start)
        cases = []
        for x in some(nx):
            for y in some(ny):
                for z in some(nz) if stack else (0,):
                    where = (near_x == x) & (near_y == y)
                    if stack:
                        where = where & (near_z == z)
                    cases.append((where, (x + y) * face + x * y * corner + (z * (1 + x) * (stack[0] + y * stack[1]) if stack else 0)))
        return waits(number, cases)

    def far_start(ref, number, shift, j, thin=False):
        first, rows = (W2 + (1 if j > 0 else 0), 1) if thin else (W2, 2)
        planes = pl.ds(P2 + 2 * mx, 2)
        copy = pltpu.make_async_remote_copy(
            src_ref=ref.at[planes, :, pl.ds(first, rows), :], dst_ref=ref.at[planes, :, pl.ds(first - 2 * j, rows), :],
            send_sem=send.at[number], recv_sem=recv.at[number],
            device_id=(lax.rem(mx + shift, nx), my + j, mz), device_id_type=MESH,
        )
        if j == 0:
            copy.start()
        else:
            pl.when(inside(0, j, 0))(copy.start)

    distances = [j for j in sorted(range(-REACH, REACH + 1), key=lambda o: -abs(o)) if abs(j) < ny]

    def column_gather(ref):
        number = used[0]
        used[0] += 1
        for j in distances:
            if j != 0:
                far_start(ref, number, 0, j)
        return waits(number, [(low_y + high_y == c, 4 * c) for c in far_counts])

    def plane_gather(ref):
        number = used[0]
        used[0] += 1
        for j in distances:
            for shift in range(nx):
                if (shift, j) != (0, 0):
                    far_start(ref, number, shift, j, abs(j) == REACH)
        thin_y = jnp.where(my >= REACH, 1, 0) + jnp.where(my + REACH < ny, 1, 0)
        cases = sorted({(min(y, REACH) + min(ny - 1 - y, REACH), (y >= REACH) + (y + REACH < ny)) for y in range(ny)})
        return waits(
            number,
            [((low_y + high_y == c) & (thin_y == t), 4 * ((1 + c) * nx - 1) - 2 * t * nx) for c, t in cases],
        )

    def row_gather(ref):
        number = used[0]
        used[0] += 1
        part = ref.at[pl.ds(P2 + 2 * mx, 2), :, pl.ds(W2 - 2 * REACH, 4 * REACH + 2), :]
        for shift in range(1, nx):
            pltpu.make_async_remote_copy(
                src_ref=part, dst_ref=part, send_sem=send.at[number], recv_sem=recv.at[number],
                device_id=(lax.rem(mx + shift, nx), my, mz), device_id_type=MESH,
            ).start()
        return waits(number, [(mx >= 0, (nx - 1) * 2 * (4 * REACH + 2))])

    def zero(ref):
        ref[...] = jnp.zeros(ref.shape, F32)

    def coarse_of(read, count, rows):
        for tile in range(2):
            for i in range(count):
                total = read(2 * i, 0, tile) + read(2 * i, 1, tile) + read(2 * i + 1, 0, tile) + read(2 * i + 1, 1, tile)
                tmp[tile, rows * i : rows * (i + 1), :] = 0.125 * total
        size = max(8, count * rows)
        lane = lanes_of((size, 128))
        pairs = [tmp[tile, 0:size, :] for tile in range(2)]
        pairs = [p + pltpu.roll(p, 127, 1) for p in pairs]
        index = (2 * lane) % 128
        out = jnp.where(lane < 64, pair_gather(pairs[0], index), pair_gather(pairs[1], index))
        tmp2[0:size, :] = out
        return [tmp2[rows * i : rows * (i + 1), :] for i in range(count)]

    def pack_edges(reads, out):
        for way, (tile, start) in enumerate(((1, 120), (0, 0))):
            packed = jnp.zeros((8, 128), F32)
            lane = lanes_of((8, 128))
            for a, read in enumerate(reads):
                for i in range(8):
                    at = 8 * i + 64 * a
                    part = pltpu.roll(read(i, tile), (at - start) % 128, 1)
                    packed = jnp.where((lane >= at) & (lane < at + 8), part, packed)
            out[way] = packed

    def edge_moves(src, dst, own, width, depth):
        moves = []
        for i, j, k in STACK:
            way, side = (0, 0) if k > 0 else (1, 1)
            rows, there = halo(j, own, width, depth)
            mine_rows = pl.ds(rows.start - own, rows.size)
            moves.append(((i, j, k), src.at[way, mine_rows, :], dst.at[side, 1 - i, there, :]))
        return moves

    def pack_coarse(out):
        lane = lanes_of((4, 128))
        for way, start in enumerate((96, 0)):
            packed = jnp.zeros((4, 128), F32)
            for i in range(4):
                part = pltpu.roll(tmp2[4 * i : 4 * i + 8, :], (32 * i - start) % 128, 1)[0:4]
                packed = jnp.where((lane >= 32 * i) & (lane < 32 * i + 32), part, packed)
            out[way, 0:4] = packed

    def unpack_coarse(src, p):
        lane = lanes_of((24, 128))
        high_end, low_start = jnp.where(mz < nz - 1, 32, 0), jnp.where(mz > 0, 96, 128)
        low = pltpu.roll(src[0, p // 4], (96 - 32 * (p % 4)) % 128, 1)
        high = pltpu.roll(src[1, p // 4], (-32 * (p % 4)) % 128, 1)
        return jnp.where(lane < high_end, high, jnp.where(lane >= low_start, low, 0.0))

    def unpack_edges(src, a, write):
        lane = lanes_of((24, 128))
        high_end, low_start = jnp.where(mz < nz - 1, 8, 0), jnp.where(mz > 0, 120, 128)
        for p in range(2 * P0 + 8):
            group, i = (0, 3 + p) if p < P0 else ((1, p - P0) if p < P0 + 8 else (2, p - P0 - 8))
            at = 8 * i + 64 * a
            low = pltpu.roll(src[0, group], (120 - at) % 128, 1)
            high = pltpu.roll(src[1, group], -at % 128, 1)
            write(p, jnp.where(lane < high_end, high, jnp.where(lane >= low_start, low, 0.0)))

    def halo(step, own, width, depth):
        if step == 0:
            return pl.ds(own, width), pl.ds(own, width)
        if step > 0:
            return pl.ds(own + width - depth, depth), pl.ds(own - depth, depth)
        return pl.ds(own, depth), pl.ds(own + width, depth)

    def fine_moves(ref, depth):
        moves = []
        for i, j, k in DIAGONAL_FIRST:
            (sp, dp), (sr, dr) = halo(i, P0, 8, depth), halo(j, W0, 8, depth)
            moves.append(((i, j, k), ref.at[sp, pl.ds(0, 2), sr, :], ref.at[dp, pl.ds(0, 2), dr, :]))
        return moves

    def coarse_moves(ref, depth, tiles):
        moves = []
        for i, j, k in DIAGONAL_FIRST:
            (sp, dp), (sr, dr) = halo(i, P1, 4, depth), halo(j, W1, 4, depth)
            if tiles:
                moves.append(((i, j, k), ref.at[sp, :, sr, :], ref.at[dp, :, dr, :]))
            else:
                moves.append(((i, j, k), ref.at[sp, sr, :], ref.at[dp, dr, :]))
        return moves

    loads = []
    for a, source in enumerate((b_ref, k_ref)):
        for tile in range(2):
            loads.append(
                pltpu.make_async_copy(
                    source.at[:, :, pl.ds(128 * tile, 128)],
                    ext.at[a, pl.ds(P0, 8), tile, pl.ds(W0, 8), :],
                    load.at[2 * a + tile],
                )
            )
            loads[-1].start()
    barrier = pltpu.get_barrier_semaphore()

    def tell(offsets, semaphore):
        for i, j, k in offsets:

            @pl.when(inside(i, j, k))
            def _():
                pl.semaphore_signal(semaphore, inc=1, device_id=(mx + i, my + j, mz + k), device_id_type=MESH)

    def hear(offsets, semaphore):
        with jax.named_scope("hear"):
            pl.semaphore_wait(semaphore, sum(jnp.where(inside(i, j, k), 1, 0) for i, j, k in offsets))

    for i, j, k in STACK + FLAT:
        ok = inside(i, j, k)
        to = tuple(jnp.where(ok, m + step, m) for m, step in ((mx, i), (my, j), (mz, k)))
        pl.semaphore_signal(barrier, inc=1, device_id=to, device_id_type=MESH)
    zero(tmp)
    zero(tmp2)
    for copy in loads:
        copy.wait()
    pack_edges([lambda i, t: ext[0, P0 + i, t, W0 : W0 + 8, :], lambda i, t: ext[1, P0 + i, t, W0 : W0 + 8, :]], edge_out)
    with jax.named_scope("barrier"):
        pl.semaphore_wait(barrier, 26)
    edges_arrive, edges_left = exchange(edge_moves(edge_out, edge_in, W0, 8, 5), 0, 0, (8, 5))
    moves = []
    for (offset, src_b, dst_b), (_, src_k, dst_k) in zip(fine_moves(ext.at[0], 4), fine_moves(ext.at[1], 5)):
        moves += [(offset, src_b, dst_b), (offset, src_k, dst_k)]
    x0_arrive, x0_left = exchange(moves, 144, 82, None)

    tell(NEXT, news.at[0])

    for ref in (redge_in, rext, bin1, bedge_in, dia1, rex1, xex1):
        zero(ref)
    own_k1 = coarse_of(lambda i, parity, t: ext[1, P0 + i, t, pl.ds(W0 + parity, 4, stride=2), :], 4, 4)
    for i, value in enumerate(own_k1):
        kin1[P1 + i, W1 : W1 + 4, :] = value
    pack_coarse(kedge_out)
    k1_arrive, k1_left = exchange(edge_moves(kedge_out, kedge_in, W1, 4, 4) + coarse_moves(kin1, 4, False), 16, 16, (4, 4))
    for ref in (va0, wa0, vb0, wb0, va1, wa1, vb1, wb1, kap2, va2, wa2, vb2, wb2, xs2):
        zero(ref)
    hear(NEXT, news.at[0])
    tell(OVER, news.at[1])
    hear(OVER, news.at[1])
    tell(FLAT, news.at[2])
    edges_arrive()

    def put(a):
        def write(p, value):
            ext[a, p, 2] = value

        return write

    unpack_edges(edge_in, 0, put(0))
    unpack_edges(edge_in, 1, put(1))
    x0_arrive()
    row = lax.broadcasted_iota(jnp.int32, (24, 128), 0)

    def planes_in(p, own, width):
        return (mx > 0) if p < own else ((mx < nx - 1) if p >= own + width else None)

    def inside_rows(p, own, width, own_row, width_row, depth):
        start = jnp.where(my > 0, own_row - depth, own_row)
        stop = jnp.where(my < ny - 1, own_row + width_row + depth, own_row + width_row)
        ok = planes_in(p, own, width)
        if ok is not None:
            stop = jnp.where(ok, stop, 0)
        return (row >= start) & (row < stop)

    for p in range(18):
        mask = inside_rows(p, P0, 8, W0, 8, 5)
        for tile in range(3):
            kap0[p, tile] = jnp.where(mask, ext[1, p, tile] * (0.5 / 30.0), 0.0)
    theta0, weights0 = chebyshev_coefs(DEGREE, FINE_LOW)
    lo, hi = P0 - 4, P0 + 12

    def start_level(level, planes, row, rows, theta, r_in, r_out, v_ref, w_ref, make_diagonal, size=3):
        kappa, diagonal, inverse = level
        for first, n in chunks(planes[0], planes[1], size):
            at = (pl.ds(first, n), slice(None), pl.ds(row, rows), slice(None))
            kap = kappa[at]
            if make_diagonal:
                dia = 128.0 * kap + stencil_sum(kappa, first, n, row, rows)
                diagonal[at] = dia
            else:
                dia = diagonal[at]
            inv = jnp.where(kap > 0.0, 1.0 / dia, 0.0)
            inverse[at] = inv
            r = jnp.where(kap > 0.0, r_in(at), 0.0)
            r_out[at] = r
            new = (theta * inv) * r
            v_ref[at] = new
            w_ref[at] = kap * new

    level0 = (kap0, dia0, inv0)
    start_level(level0, (lo, hi), 4, 16, theta0, lambda at: ext[(0,) + at], res0, va0, wa0, True, FINE)

    def own0(ref):
        return ref[P0 : P0 + 8, 0:2, W0 : W0 + 8, :]

    xs0[...] = own0(va0)
    here, there = (va0, wa0), (vb0, wb0)

    def smooth0(step, r_in):
        nonlocal here, there
        apply(level0, here, r_in, res0, (P0 - 3 + step, P0 + 11 - step), 4, 16, weights0[step], there, FINE)
        xs0[...] += own0(there[0])
        here, there = there, here

    smooth0(0, lambda at: res0[at])
    smooth0(1, lambda at: res0[at])

    k1_arrive()
    for p in range(12):
        mask = inside_rows(p, P1, 4, W1, 4, 4)
        kap1[p, 0] = jnp.where(mask, kin1[p] * (0.125 / 30.0), 0.0)
        kap1[p, 1] = jnp.where(mask, unpack_coarse(kedge_in, p) * (0.125 / 30.0), 0.0)
    for first, n in chunks(P1, P1 + 4, 2):
        at = (pl.ds(first, n), slice(None), pl.ds(W1, 8), slice(None))
        value = 128.0 * kap1[at] + stencil_sum(kap1, first, n, W1, 8)
        dia1[first : first + n, :, W1 : W1 + 4, :] = value[:, :, 0:4]
    hear(FLAT, news.at[2])
    d1_arrive, d1_left = exchange(coarse_moves(dia1, 4, True), 32, 32, None)
    smooth0(2, lambda at: res0[at])

    def put_rext(first, n, r):
        rext[0, pl.ds(first, n), 0:2, W0 : W0 + 8, :] = r[:, 0:2]

    apply(level0, here, lambda at: res0[at], put_rext, (P0, P0 + 8), W0, 8, None, None, FINE)

    own_b1 = coarse_of(lambda i, parity, t: rext[0, P0 + i, t, pl.ds(W0 + parity, 4, stride=2), :], 4, 4)
    for i, value in enumerate(own_b1):
        bin1[P1 + i, W1 : W1 + 4, :] = value
    pack_coarse(bedge_out)
    b1_arrive, b1_left = exchange(edge_moves(bedge_out, bedge_in, W1, 4, 4) + coarse_moves(bin1, 4, False), 16, 16, (4, 4))
    own_k2 = coarse_of(lambda i, parity, t: kap1[P1 + i, t, pl.ds(W1 + parity, 2, stride=2), :], 2, 2)
    for i, value in enumerate(own_k2):
        kin2[P2 + 2 * mx + i, 0, W2 : W2 + 2, :] = 0.25 * value
    k2_arrive, k2_left = column_gather(kin2)
    pack_edges([lambda i, t: rext[0, P0 + i, t, W0 : W0 + 8, :]], redge_out)
    edges_left()
    x0_left()
    k1_left()
    d1_arrive()
    d1_left()
    b1_arrive()
    for p in range(12):
        res1[p, 0] = bin1[p]
        res1[p, 1] = unpack_coarse(bedge_in, p)
    level1 = (kap1, dia1, inv1)
    start_level(level1, (0, 12), 4, 16, theta0, lambda at: res1[at], res1, va1, wa1, False)

    def own1(ref):
        return ref[P1 : P1 + 4, :, W1 : W1 + 8, :]

    xs1[...] = own1(va1)
    here, there = (va1, wa1), (vb1, wb1)
    for step in range(3):
        at_row, rows = ((4, 16), (6, 8), (7, 8))[step]
        apply(level1, here, lambda at: res1[at], res1, (P1 - 3 + step, P1 + 7 - step), at_row, rows, weights0[step], there)
        xs1[...] += own1(there[0])
        here, there = there, here

    def put_rex1(first, n, r):
        rex1[pl.ds(first, n), :, W1 : W1 + 4, :] = r[:, :, 0:4]

    apply(level1, here, lambda at: res1[at], put_rex1, (P1, P1 + 4), W1, 8, None)

    own_b2 = coarse_of(lambda i, parity, t: rex1[P1 + i, t, pl.ds(W1 + parity, 2, stride=2), :], 2, 2)
    for i, value in enumerate(own_b2):
        bin2[P2 + 2 * mx + i, 0, W2 : W2 + 2, :] = value
    b2_arrive, b2_left = plane_gather(bin2)
    k2_arrive()
    m2_arrive, m2_left = row_gather(kin2)
    r1_arrive, r1_left = exchange(coarse_moves(rex1, 3, True), 24, 18, None)
    r0_arrive, r0_left = exchange(edge_moves(redge_out, redge_in, W0, 8, 4) + fine_moves(rext.at[0], 4), 64, 32, (8, 4))
    k2_left()
    b1_left()
    m2_arrive()
    m2_left()
    full = 2 * nx
    at_row = lax.broadcasted_iota(jnp.int32, (full, 1, 24, 128), 2) + (8 - W2)
    start, stop = jnp.maximum(-2 * REACH, -2 * my), jnp.minimum(2 * REACH + 2, 2 * (ny - my))
    window = (slice(P2, P2 + full), slice(None), slice(8, 32), slice(None))
    kap2[window] = jnp.where((at_row >= start) & (at_row < stop), kin2[window], 0.0)
    theta2, weights2 = chebyshev_coefs(COARSE_DEGREE, COARSE_LOW)
    level2 = (kap2, dia2, inv2)
    b2_arrive()
    start_level(level2, (P2, P2 + full), 8, 24, theta2, lambda at: bin2[at], res2, va2, wa2, True, 1)
    near = (slice(P2, P2 + full), slice(None), slice(W2 - 3, W2 + 5), slice(None))
    xs2[near] = va2[near]
    here, there = (va2, wa2), (vb2, wb2)
    for step in range(COARSE_DEGREE - 1):
        at_row, rows = (8, 24) if step == 0 else ((W2 - 7, 16) if step < 5 else (W2 - 3, 8))
        apply(level2, here, lambda at: res2[at], res2, (P2, P2 + full), at_row, rows, weights2[step], there, 1)
        xs2[near] += there[0][near]
        here, there = there, here

    half = lanes_of((8, 128)) // 2
    for j in range(6):
        coarse = xs2[P2 + 2 * mx - 2 + j, 0, W2 - 2 : W2 + 6, :]
        for tile in range(2):
            value = pair_gather(coarse, half + 64 * tile)[0:6]
            for e in range(2):
                for parity in range(2):
                    va1[2 * j + e, tile, pl.ds(W1 - 4 + parity, 6, stride=2), :] = value
    for first, n in chunks(0, 12, 2):
        wa1[first : first + n] = kap1[first : first + n] * va1[first : first + n]
    xs1[...] += own1(va1)
    r1_arrive()
    here, there = (va1, wa1), (vb1, wb1)
    apply(level1, here, lambda at: rex1[at], res1, (P1 - 3, P1 + 7), 4, 16, (None, theta0), there)
    xs1[...] += own1(there[0])
    here, there = there, here
    for step in range(3):
        at_row = (6, 7, 8)[step]
        apply(level1, here, lambda at: res1[at], res1, (P1 - 2 + step, P1 + 6 - step), at_row, 8, weights0[step], there)
        xs1[...] += own1(there[0])
        here, there = there, here
    xex1[P1 : P1 + 4, :, W1 : W1 + 4, :] = xs1[:, :, 0:4, :]
    x1_arrive, x1_left = exchange(coarse_moves(xex1, 3, True), 24, 18, None)
    b2_left()
    r1_left()
    r0_left()
    r0_arrive()

    def put_rext2(p, value):
        rext[0, p, 2] = value

    unpack_edges(redge_in, 0, put_rext2)
    x1_arrive()
    lane = lanes_of((8, 128))
    ends = jnp.where(lane < 64, half, half + 64)
    for p in range(1, 11):
        for source_row, keep in ((W1 - 4, 8), (W1 + 4, 4)):
            for tile, source_tile, index in ((0, 0, half), (1, 0, half + 64), (2, 1, ends)):
                value = pair_gather(xex1[p, source_tile, source_row : source_row + 8, :], index)[0:keep]
                for q in (2 * p - 3, 2 * p - 2):
                    if 0 <= q < 18:
                        for parity in range(2):
                            va0[q, tile, pl.ds(2 * (source_row - 4) + parity, keep, stride=2), :] = value
    for first, n in chunks(0, 18, 2):
        wa0[first : first + n] = kap0[first : first + n] * va0[first : first + n]
    xs0[...] += own0(va0)
    here, there = (va0, wa0), (vb0, wb0)
    apply(level0, here, lambda at: rext[(0,) + at], res0, (lo, hi), 4, 16, (None, theta0), there, FINE)
    xs0[...] += own0(there[0])
    here, there = there, here
    for step in range(3):
        smooth0(step, lambda at: res0[at])

    def put_out(first, n, r):
        for tile in range(2):
            r_ref[first - P0 : first - P0 + n, :, 128 * tile : 128 * tile + 128] = r[:, tile]

    apply(level0, here, lambda at: res0[at], put_out, (P0, P0 + 8), W0, 8, None, None, FINE)
    for tile in range(2):
        x_ref[:, :, 128 * tile : 128 * tile + 128] = xs0[:, tile]
    x1_left()


def solution(mesh):
    sizes = tuple(mesh.shape[axis] for axis in ("gx", "gy", "gz"))

    def step(conductivity, source):
        def vmem(*shape):
            return pltpu.VMEM(shape, F32)

        level0, level1, level2 = (18, 3, 24, 128), (12, 2, 24, 128), (12, 1, 40, 128)
        sems = 11
        shape = jax.ShapeDtypeStruct(conductivity.shape, F32)
        return pl.pallas_call(
            lambda *refs: kernel(sizes, *refs),
            name="cycle",
            out_shape=(shape, shape),
            in_specs=[pl.BlockSpec(memory_space=pltpu.HBM)] * 2,
            out_specs=(pl.BlockSpec(memory_space=pltpu.VMEM),) * 2,
            scratch_shapes=[
                vmem(2, *level0), vmem(2, 3, 24, 128), vmem(2, 8, 128), vmem(2, 3, 24, 128), vmem(2, 8, 128), vmem(1, *level0),
                *[vmem(*level0) for _ in range(4)], vmem(19, 3, 24, 128), *[vmem(*level0) for _ in range(3)], vmem(8, 2, 8, 128),
                vmem(12, 24, 128), vmem(12, 24, 128), *[vmem(*s) for s in 2 * ((2, 3, 24, 128), (2, 8, 128))], *[vmem(*level1) for _ in range(10)], vmem(4, 2, 8, 128),
                *[vmem(*level2) for _ in range(11)],
                vmem(2, 24, 128), vmem(24, 128), vmem(1152, 128),
                pltpu.SemaphoreType.DMA((sems,)), pltpu.SemaphoreType.DMA((sems,)), pltpu.SemaphoreType.DMA((4,)),
                pltpu.SemaphoreType.REGULAR((3,)),
            ],
            compiler_params=pltpu.CompilerParams(
                collective_id=0, has_side_effects=True, vmem_limit_bytes=50 * 1024 * 1024
            ),
        )(*(pltpu.with_memory_space_constraint(v, pltpu.HBM) for v in (conductivity, source)))

    spec = P("gx", "gy", "gz")
    return jax.shard_map(step, mesh=mesh, in_specs=(spec, spec), out_specs=(spec, spec), check_vma=False)
```
